32 devices in a mesh: dp: 8 (over y, x, core), expert: 4 (over z).
Axes of the slice: x: 2, y: 2, z: 4, core: 2. Of those that a mesh axis runs over, the one named last changes fastest.
Arguments:
- tokens: bfloat16 [4096, 2048], P(('dp', 'expert')), may hold values from -6 to 6
- routes: int32 [4096, 2], P(('dp', 'expert')), may hold values from 0 to 3, as said below
- grad_hidden: bfloat16 [4096, 2, 768], P(('dp', 'expert')), may hold values from -1.1953125 to 1.1953125
- w_gate: bfloat16 [4, 2048, 768], P('expert'), may hold values from -0.125 to 0.125
- w_up: bfloat16 [4, 2048, 768], P('expert'), may hold values from -0.125 to 0.125
Outputs:
- grad_tokens: bfloat16 [4096, 2048], P(('dp', 'expert'))
- grad_gate: float32 [4, 2048, 768], P('expert', 'dp')
- grad_up: float32 [4, 2048, 768], P('expert', 'dp')
The draws below stay inside these ranges and needn't reach their ends.
Inputs may be any that keep to these rules, and one draw needn't show every extreme that they name: `routes`: each row names 2 different experts. In each data group 2 experts are hot, the same for all rows of the group: in the rows of one device each hot expert of its group is named more often than every other expert and at most 73 times, every other expert at most 64 times. In the rows of every device some expert is named exactly 64 times; in the rows of some device a hot expert is named exactly 73 times. Every expert is hot in some data group. The indices of a group's two hot experts never differ by 2.
All inputs are finite; a program needn't handle non-finite values.
Results may differ from the reference program's by a relative error of at most 0.012.
Values may be sent and summed in bfloat16 or wider, within the bound.
A program may use at most 128 MiB of HBM per device.

```python
import jax
import jax.numpy as jnp
from jax import lax

D = 2048
FF = 768
TOP = 2
TOK_DEV = 128
EXPERTS = 4
DATA_GROUPS = 8
ROW_TOKENS = 512
TOKENS = 4096
COLD = 64
HMAX = 73
N_EXPERT = 4


def draw_routes(key, part):
    nblock = TOKENS // TOK_DEV
    pair_count = TOK_DEV * TOP
    cold_top = pair_count // EXPERTS
    cold_floor = cold_top - 2 - cold_top // 8
    subkeys = jax.random.split(key, 9)
    expert_ids = jnp.arange(EXPERTS, dtype=jnp.int32)
    block_ids = jnp.arange(nblock, dtype=jnp.int32)
    group_ids = block_ids // EXPERTS
    rotation = jax.random.randint(subkeys[0], (), 0, EXPERTS)
    first_hot = (rotation + group_ids) % EXPERTS
    group_offset = jax.random.randint(subkeys[1], (DATA_GROUPS,), 1, EXPERTS // 2)
    offset = group_offset[group_ids]
    second_hot = (first_hot + offset) % EXPERTS
    hot_one = expert_ids[None, :] == first_hot[:, None]
    hot_two = expert_ids[None, :] == second_hot[:, None]
    hot_flag = hot_one | hot_two
    load_table = jax.random.randint(subkeys[2], (nblock, EXPERTS), cold_floor, cold_top - 1)
    scores = jax.random.randint(subkeys[3], (nblock, EXPERTS), 0, 1 << 20) * EXPERTS + expert_ids[None, :]
    scores = jnp.where(hot_flag, -1, scores)
    forced = jnp.argmax(scores, axis=1).astype(jnp.int32)
    special = jax.random.randint(subkeys[4], (), 0, nblock)
    at_special = block_ids == special
    load_table = jnp.where(at_special[:, None], cold_floor, load_table)
    load_table = jnp.where(expert_ids[None, :] == forced[:, None], cold_top, load_table)
    load_table = jnp.where(hot_flag, 0, load_table)
    hot_total = pair_count - jnp.sum(load_table, axis=1)
    spread = jnp.minimum((hot_total - 2 * cold_top - 2) // 2, cold_top // 4)
    extra_load = jax.random.randint(subkeys[5], (nblock,), 0, spread + 1)
    extra_load = jnp.where(at_special, spread, extra_load)
    larger = (hot_total + 1) // 2 + extra_load
    smaller = hot_total - larger
    flipped = jax.random.randint(subkeys[6], (nblock,), 0, 2) == 1
    load_one = jnp.where(flipped, smaller, larger)
    load_two = jnp.where(flipped, larger, smaller)
    load_table = load_table + jnp.where(hot_one, load_one[:, None], 0) + jnp.where(hot_two, load_two[:, None], 0)

    def tickets(counts):
        return jnp.repeat(expert_ids, counts, total_repeat_length=pair_count)
    ticket_rows = jax.vmap(tickets)(load_table)
    pair_rows = jnp.stack([ticket_rows[:, :TOK_DEV], ticket_rows[:, TOK_DEV:]], axis=2)
    swapped = jax.random.randint(subkeys[7], (nblock, TOK_DEV, 1), 0, 2) == 1
    pair_rows = jnp.where(swapped, pair_rows[:, :, ::-1], pair_rows)

    def shuffle(block_key):
        return jax.random.permutation(block_key, TOK_DEV)
    token_order = jax.vmap(shuffle)(jax.random.split(subkeys[8], nblock))
    pair_rows = jnp.take_along_axis(pair_rows, token_order[:, :, None], axis=1)
    return pair_rows.reshape(TOKENS, TOP).astype(jnp.int32)


def shard_levels(key, shape, cuts, least, high):
    factor_of = 1.0
    for position, parts in cuts:
        draws = jax.random.uniform(jax.random.fold_in(jax.random.fold_in(key, 6), position), (parts,), jnp.float32, least / len(cuts), high / len(cuts))
        factor_of = factor_of * jnp.repeat(jnp.exp(draws), shape[position] // parts).reshape((-1,) + (1,) * (len(shape) - 1 - position))
    return factor_of


def normal_values(rng, extent, scale, limit, cuts=(), kind=jnp.bfloat16):
    result = jax.random.normal(rng, extent, jnp.float32) * scale
    if len(cuts) > 0:
        result = shard_levels(rng, extent, cuts, -0.22, 0.18) * result
    return jnp.clip(result, min=-limit, max=limit).astype(kind)


def setup_inputs(seed: int = 0) -> dict:
    streams_of = jax.random.split(jax.random.key(seed), 6)
    return {
        "tokens": normal_values(streams_of[0], (TOKENS, D), 1.0, 6.0, ((0, 32),)),
        "routes": draw_routes(jax.random.fold_in(streams_of[5], 71), 0),
        "grad_hidden": normal_values(streams_of[2], (TOKENS, TOP, FF), 0.2, 1.1953125, ((0, 32),)),
        "w_gate": normal_values(streams_of[3], (EXPERTS, D, FF), D ** -0.5, 0.125, ((0, 4),)),
        "w_up": normal_values(streams_of[4], (EXPERTS, D, FF), D ** -0.5, 0.125, ((0, 4),)),
    }


def expert_grads(rows_x, rows_dh, gate_w, up_w, spill_rows):
    gate_act = jnp.dot(rows_x, gate_w, preferred_element_type=jnp.float32)
    up_act = jnp.dot(rows_x, up_w, preferred_element_type=jnp.float32)
    gate_sig = jax.nn.sigmoid(gate_act)
    grad_wide = rows_dh.astype(jnp.float32)
    gate_delta = (grad_wide * up_act * gate_sig * (1.0 + gate_act * (1.0 - gate_sig))).astype(jnp.bfloat16)
    up_delta = (grad_wide * gate_act * gate_sig).astype(jnp.bfloat16)
    back_rows = lax.dot_general(gate_delta, gate_w, (((1,), (1,)), ((), ())), preferred_element_type=jnp.float32)
    back_rows = back_rows + lax.dot_general(up_delta, up_w, (((1,), (1,)), ((), ())), preferred_element_type=jnp.float32)
    zero_delta = jnp.zeros_like(gate_delta)
    gate_keep = jnp.where(spill_rows[:, None], zero_delta, gate_delta)
    gate_spill = jnp.where(spill_rows[:, None], gate_delta, zero_delta)
    up_keep = jnp.where(spill_rows[:, None], zero_delta, up_delta)
    up_spill = jnp.where(spill_rows[:, None], up_delta, zero_delta)
    dims = (((0,), (0,)), ((), ()))
    grads = tuple(lax.dot_general(rows_x, delta, dims, preferred_element_type=jnp.float32) for delta in (gate_keep, gate_spill, up_keep, up_spill))
    return back_rows.astype(jnp.bfloat16), grads


def reference(tokens, routes, grad_hidden, w_gate, w_up):
    row_pairs = ROW_TOKENS * TOP
    block_rows = 64
    slot_count = row_pairs + EXPERTS * block_rows
    block_count = slot_count // block_rows
    limit_rows = COLD + (HMAX - COLD + 1) // 2
    token_groups = tokens.reshape(DATA_GROUPS, ROW_TOKENS, D)
    route_groups = routes.reshape(DATA_GROUPS, row_pairs)
    grad_groups = grad_hidden.reshape(DATA_GROUPS, row_pairs, FF)
    expert_ids = jnp.arange(EXPERTS, dtype=jnp.int32)

    def one_group(totals, items):
        group_tokens, group_routes, group_grads = items
        device_routes = group_routes.reshape(N_EXPERT, TOK_DEV * TOP)
        member = (device_routes[:, :, None] == expert_ids[None, None, :]).astype(jnp.int32)
        ranked = jnp.sum(jnp.cumsum(member, axis=1) * member, axis=2) - 1
        spill_flag = (ranked >= limit_rows).reshape(row_pairs)
        padded_spill = jnp.concatenate([spill_flag, jnp.zeros((1,), bool)], axis=0)
        counts = jnp.sum((group_routes[:, None] == expert_ids[None, :]).astype(jnp.int32), axis=0)
        padded = (counts + block_rows - 1) // block_rows * block_rows
        offsets = jnp.cumsum(padded) - padded
        starts = jnp.cumsum(counts) - counts
        ordering = jnp.argsort(group_routes, stable=True).astype(jnp.int32)
        sorted_ids = group_routes[ordering]
        slot_of = offsets[sorted_ids] + jnp.arange(row_pairs, dtype=jnp.int32) - starts[sorted_ids]
        slot_table = jnp.full((slot_count,), row_pairs, jnp.int32).at[slot_of].set(ordering)
        end_of = offsets + padded
        block_start = jnp.arange(block_count, dtype=jnp.int32) * block_rows
        block_owner = jnp.minimum(jnp.sum((block_start[:, None] >= end_of[None, :]).astype(jnp.int32), axis=1), EXPERTS - 1)
        padded_tokens = jnp.concatenate([group_tokens, jnp.zeros((1, D), group_tokens.dtype)], axis=0)
        padded_grads = jnp.concatenate([group_grads, jnp.zeros((1, FF), group_grads.dtype)], axis=0)

        def one_block(accums, block_index):
            picked = lax.dynamic_slice_in_dim(slot_table, block_index * block_rows, block_rows)
            tok_index = jnp.where(picked < row_pairs, picked // TOP, ROW_TOKENS).astype(jnp.int32)
            rows_x = padded_tokens[tok_index]
            rows_dh = padded_grads[picked]
            spill_rows = padded_spill[picked]
            expert_now = block_owner[block_index]
            back_rows, grads = expert_grads(rows_x, rows_dh, w_gate[expert_now], w_up[expert_now], spill_rows)
            new_accums = tuple(acc.at[expert_now].add(part) for acc, part in zip(accums, grads))
            return new_accums, back_rows

        zero_grads = jnp.zeros((EXPERTS, D, FF), jnp.float32)
        accums, pair_backs = lax.scan(one_block, (zero_grads, zero_grads, zero_grads, zero_grads), jnp.arange(block_count, dtype=jnp.int32))
        pair_back = jnp.zeros((row_pairs + 1, D), jnp.bfloat16).at[slot_table].set(pair_backs.reshape(slot_count, D))[:row_pairs]
        rounded = [lax.optimization_barrier(acc.astype(jnp.bfloat16)).astype(jnp.float32) for acc in accums]
        return (totals[0] + rounded[0] + rounded[1], totals[1] + rounded[2] + rounded[3]), pair_back

    zero_grads = jnp.zeros((EXPERTS, D, FF), jnp.float32)
    grads, pair_backs = lax.scan(one_group, (zero_grads, zero_grads), (token_groups, route_groups, grad_groups))
    pair_backs = lax.optimization_barrier(pair_backs)
    grad_tokens = jnp.sum(pair_backs.reshape(TOKENS, TOP, D).astype(jnp.float32), axis=1).astype(jnp.bfloat16)
    return grad_tokens, grads[0], grads[1]
```

```python
import functools

import jax
import jax.numpy as jnp
from jax import lax
from jax.experimental import pallas as pl
from jax.experimental.pallas import tpu as pltpu
from jax.sharding import PartitionSpec as P

MESH = pl.DeviceIdType.MESH
BF = jnp.bfloat16
F32 = jnp.float32


def dot(a, b, da, db):
    return lax.dot_general(a, b, (((da,), (db,)), ((), ())), preferred_element_type=F32)


def rs_plan(bits):
    orders = (tuple(range(bits)), (0,) + tuple(range(bits - 1, 0, -1)))
    index = {}
    for which, order in enumerate(orders):
        done = 1
        for bit in order[1:]:
            flag = 1 << bit
            for mask in range(1 << bits):
                if mask & done or mask & flag:
                    continue
                index[which, bit, mask] = len(index)
            done |= flag
    return orders, index


def kernel(
    groups, ways, cap, tok_ref, rt_ref, gh0_ref, gh1_ref, wg_hbm, wu_hbm,
    out_tok, out_gate, out_up,
    wg, wu, pick, send, rows, delta, back, ret, core_send, core_recv, hop_send, hop_recv, acc,
    w_sem, z_ssem, z_rsem, b_ssem, b_rsem, c_ssem, c_rsem, h_ssem, h_rsem,
):
    features = tok_ref.shape[1]
    toks = tok_ref.shape[0]
    hidden = gh0_ref.shape[1]
    block = features // ways
    bits = ways.bit_length() - 1
    orders, index = rs_plan(bits)
    me = lax.axis_index("expert")
    dp = lax.axis_index("dp")
    my_bits = [lax.rem(dp // (1 << b), 2) for b in range(bits)]

    def peer_dp(mask):
        total = 0
        for b in range(bits):
            bit = 1 - my_bits[b] if mask >> b & 1 else my_bits[b]
            total = total + bit * (1 << b)
        return total

    load_g = pltpu.make_async_copy(wg_hbm, wg, w_sem.at[0])
    load_u = pltpu.make_async_copy(wu_hbm, wu, w_sem.at[1])
    load_g.start()
    load_u.start()

    barrier = pltpu.get_barrier_semaphore()
    for off in range(1, groups):
        pl.semaphore_signal(
            barrier, inc=1, device_id={"expert": lax.rem(me + off, groups)}, device_id_type=MESH
        )
    for b in range(bits):
        pl.semaphore_signal(
            barrier, inc=1, device_id={"dp": peer_dp(1 << b)}, device_id_type=MESH
        )

    r0 = rt_ref[0:1, :]
    r1 = rt_ref[1:2, :]
    wide = max(groups, 8)
    ids = lax.broadcasted_iota(jnp.int32, (wide, toks), 0)
    is0 = (ids == r0).astype(F32)
    is1 = (ids == r1).astype(F32)
    before = (
        lax.broadcasted_iota(jnp.int32, (toks, toks), 0)
        < lax.broadcasted_iota(jnp.int32, (toks, toks), 1)
    ).astype(F32).astype(BF)
    earlier = dot((is0 + is1).astype(BF), before, 1, 0)
    pos0 = r0.astype(F32) * cap + jnp.sum(is0 * earlier, axis=0, keepdims=True)
    pos1 = r1.astype(F32) * cap + jnp.sum(is1 * earlier, axis=0, keepdims=True)
    slot = lax.broadcasted_iota(jnp.int32, (groups * cap, toks), 0).astype(F32)
    m0 = (slot == pos0).astype(F32)
    m1 = (slot == pos1).astype(F32)
    pick[...] = (m0 + m1).astype(BF)
    send[:, features:] = (
        dot(m0.astype(BF), gh0_ref[...], 1, 0) + dot(m1.astype(BF), gh1_ref[...], 1, 0)
    ).astype(BF)
    step = 512
    for c in range(0, features, step):
        send[:, c : c + step] = dot(pick[...], tok_ref[:, c : c + step], 1, 0).astype(BF)

    pl.semaphore_wait(barrier, groups - 1 + bits)

    def span(i):
        return pl.ds(pl.multiple_of(i * cap, cap), cap)

    def exchange(src, dst, ssem, rsem):
        sends, recvs = [], []
        for off in range(1, groups):
            to = lax.rem(me + off, groups)
            frm = lax.rem(me + groups - off, groups)
            sends.append(pltpu.make_async_remote_copy(
                src_ref=src.at[span(to)], dst_ref=dst.at[span(me)],
                send_sem=ssem.at[off], recv_sem=rsem.at[off],
                device_id={"expert": to}, device_id_type=MESH))
            recvs.append(pltpu.make_async_remote_copy(
                src_ref=src.at[span(frm)], dst_ref=dst.at[span(frm)],
                send_sem=ssem.at[off], recv_sem=rsem.at[off],
                device_id={"expert": frm}, device_id_type=MESH))
        for copy in sends:
            copy.start()
        return sends, recvs

    out_sends, out_recvs = exchange(send, rows, z_ssem, z_rsem)
    rows[span(me), :] = send[span(me), :]
    load_g.wait()
    load_u.wait()
    for copy in out_recvs:
        copy.wait_recv()

    tile = 256

    def forward(f, carry):
        cols = pl.ds(pl.multiple_of(f * tile, tile), tile)
        ucols = pl.ds(pl.multiple_of(f * tile + hidden, tile), tile)
        dcols = pl.ds(pl.multiple_of(f * tile + features, tile), tile)
        x = rows[:, 0:features]
        gate = dot(x, wg[:, cols], 1, 0)
        up = dot(x, wu[:, cols], 1, 0)
        sig = jax.nn.sigmoid(gate)
        grad = rows[:, dcols].astype(F32)
        delta[:, cols] = (grad * up * sig * (1.0 + gate * (1.0 - sig))).astype(BF)
        delta[:, ucols] = (grad * gate * sig).astype(BF)
        return carry

    lax.fori_loop(0, hidden // tile, forward, 0)

    def weight_block(mask):
        start = pl.multiple_of(peer_dp(mask) * block, block)
        return dot(rows[:, pl.ds(start, block)], delta[...], 0, 0)

    core_sends = {}
    for mask in range(ways - 1, 0, -2):
        place = mask >> 1
        core_send[place] = weight_block(mask).astype(BF)
        copy = pltpu.make_async_remote_copy(
            src_ref=core_send.at[place], dst_ref=core_recv.at[place],
            send_sem=c_ssem.at[place], recv_sem=c_rsem.at[place],
            device_id={"dp": peer_dp(1)}, device_id_type=MESH)
        copy.start()
        core_sends[place] = copy

    def backward(d, carry):
        cols = pl.ds(pl.multiple_of(d * tile, tile), tile)
        back[:, cols] = (
            dot(delta[:, 0:hidden], wg[cols, :], 1, 1)
            + dot(delta[:, hidden:], wu[cols, :], 1, 1)
        ).astype(BF)
        return carry

    lax.fori_loop(0, features // tile, backward, 0)
    back_sends, back_recvs = exchange(back, ret, b_ssem, b_rsem)
    ret[span(me), :] = back[span(me), :]

    hop_sends = []

    def hop(which, bit, mask, value):
        at = index[which, bit, mask ^ (1 << bit)]
        hop_send[at] = value.astype(BF)
        copy = pltpu.make_async_remote_copy(
            src_ref=hop_send.at[at], dst_ref=hop_recv.at[at],
            send_sem=h_ssem.at[at], recv_sem=h_rsem.at[at],
            device_id={"dp": peer_dp(1 << bit)}, device_id_type=MESH)
        copy.start()
        hop_sends.append(copy)

    def arrived(which, bit, mask):
        at = index[which, bit, mask]
        pltpu.make_async_remote_copy(
            src_ref=hop_send.at[at], dst_ref=hop_recv.at[at],
            send_sem=h_ssem.at[at], recv_sem=h_rsem.at[at],
            device_id={"dp": peer_dp(1 << bit)}, device_id_type=MESH).wait_recv()
        return hop_recv[at].astype(F32)

    for mask in range(ways - 2, -1, -2):
        place = mask >> 1
        core_sends[place].wait_recv()
        total = weight_block(mask) + core_recv[place].astype(F32)
        for which in range(2):
            part = total[:, which * hidden : (which + 1) * hidden]
            bit = orders[which][1]
            if mask >> bit & 1:
                hop(which, bit, mask, part)
            else:
                acc[which, place] = part

    for level in range(2, bits):
        for mask in range(ways - 2, -1, -2):
            for which in range(2):
                order = orders[which]
                fixed = sum(1 << b for b in order[:level])
                if mask & fixed:
                    continue
                value = acc[which, mask >> 1] + arrived(which, order[level - 1], mask)
                if mask >> order[level] & 1:
                    hop(which, order[level], mask, value)
                else:
                    acc[which, mask >> 1] = value

    for copy in back_recvs:
        copy.wait_recv()
    for c in range(0, features, step):
        out_tok[:, c : c + step] = dot(pick[...], ret[:, c : c + step], 0, 0).astype(BF)
    out_gate[...] = acc[0, 0] + arrived(0, orders[0][-1], 0)
    out_up[...] = acc[1, 0] + arrived(1, orders[1][-1], 0)

    for copy in out_sends + back_sends + list(core_sends.values()) + hop_sends:
        copy.wait_send()


def gather_plan(bits):
    if bits > 2:
        orders = (tuple(range(1, bits)) + (0,), tuple(range(bits - 1, 0, -1)) + (0,))
    else:
        orders = (tuple(range(bits - 1, -1, -1)),) * 2
    via = {}
    for part, order in enumerate(orders):
        for mask in range(1, 1 << bits):
            via[mask, part] = [b for b in order if mask >> b & 1][-1]
    masks = sorted(range(1, 1 << bits), key=lambda mask: (bin(mask).count("1"), mask))
    return masks, via


def gather_kernel(
    groups, ways, cap, tok_ref, rt_ref, gh0_ref, gh1_ref, wg_hbm, wu_hbm,
    out_tok, out_gate, out_up,
    wg, wu, pick, pick0, pick1, sx, sd, rx, rd, dg, xg, sback, ret, acc,
    w_sem, x_ss, x_rs, d_ss, d_rs, b_ss, b_rs, g_ss, g_rs, c_ss, c_rs,
):
    features = tok_ref.shape[1]
    toks = tok_ref.shape[0]
    hidden = gh0_ref.shape[1]
    block = features // ways
    bits = ways.bit_length() - 1
    masks, via = gather_plan(bits)
    me = lax.axis_index("expert")
    dp = lax.axis_index("dp")

    def flip(value, mask, count):
        total = 0
        for b in range(count):
            bit = lax.rem(value // (1 << b), 2)
            if mask >> b & 1:
                bit = 1 - bit
            total = total + bit * (1 << b)
        return total

    partner = [flip(me, k, groups.bit_length() - 1) for k in range(groups)]
    peer = [flip(dp, m, bits) for m in range(ways)]

    load_g = pltpu.make_async_copy(wg_hbm, wg, w_sem.at[0])
    load_u = pltpu.make_async_copy(wu_hbm, wu, w_sem.at[1])
    load_g.start()
    load_u.start()

    barrier = pltpu.get_barrier_semaphore()
    for k in range(1, groups):
        pl.semaphore_signal(barrier, inc=1, device_id={"expert": partner[k]}, device_id_type=MESH)
    for m in range(1, ways):
        pl.semaphore_signal(barrier, inc=1, device_id={"dp": peer[m]}, device_id_type=MESH)

    r0 = rt_ref[0:1, :]
    r1 = rt_ref[1:2, :]
    wide = max(groups, 8)
    ids = lax.broadcasted_iota(jnp.int32, (wide, toks), 0)
    is0 = (ids == r0).astype(F32)
    is1 = (ids == r1).astype(F32)
    before = (
        lax.broadcasted_iota(jnp.int32, (toks, toks), 0)
        < lax.broadcasted_iota(jnp.int32, (toks, toks), 1)
    ).astype(F32).astype(BF)
    earlier = dot((is0 + is1).astype(BF), before, 1, 0)
    pos0 = r0.astype(F32) * cap + jnp.sum(is0 * earlier, axis=0, keepdims=True)
    pos1 = r1.astype(F32) * cap + jnp.sum(is1 * earlier, axis=0, keepdims=True)
    slot = lax.broadcasted_iota(jnp.int32, (groups * cap, toks), 0).astype(F32)
    m0 = (slot == pos0).astype(F32)
    m1 = (slot == pos1).astype(F32)
    pick0[...] = m0.astype(BF)
    pick1[...] = m1.astype(BF)
    pick[...] = (m0 + m1).astype(BF)

    def span(i):
        return pl.ds(pl.multiple_of(i * cap, cap), cap)

    def to_expert(src, dst, ssem, rsem, k):
        return pltpu.make_async_remote_copy(
            src_ref=src.at[k], dst_ref=dst.at[k], send_sem=ssem.at[k], recv_sem=rsem.at[k],
            device_id={"expert": partner[k]}, device_id_type=MESH)

    pending = []
    x_copy, d_copy, b_copy = {}, {}, {}
    step = 512
    greeted = False
    for k in list(range(1, groups)) + [0]:
        rows_x = sx if k else rx
        rows_d = sd if k else rd
        for c in range(0, features, step):
            rows_x[k, :, c : c + step] = dot(
                pick[span(partner[k]), :], tok_ref[:, c : c + step], 1, 0).astype(BF)
        if not greeted:
            pl.semaphore_wait(barrier, groups - 1 + ways - 1)
            greeted = True
        if k:
            x_copy[k] = to_expert(sx, rx, x_ss, x_rs, k)
            x_copy[k].start()
        rows_d[k] = (
            dot(pick0[span(partner[k]), :], gh0_ref[...], 1, 0)
            + dot(pick1[span(partner[k]), :], gh1_ref[...], 1, 0)
        ).astype(BF)
        if k:
            d_copy[k] = to_expert(sd, rd, d_ss, d_rs, k)
            d_copy[k].start()
            pending += [x_copy[k], d_copy[k]]

    tile = 256

    def place(mask):
        return pl.ds(mask * cap, cap)

    def part_cols(part):
        return pl.ds(part * hidden, hidden)

    def delta_copy(k, mask, part):
        bit = via[mask, part]
        return pltpu.make_async_remote_copy(
            src_ref=dg.at[k, place(mask ^ (1 << bit)), part_cols(part)],
            dst_ref=dg.at[k, place(mask), part_cols(part)],
            send_sem=c_ss.at[k, mask, part], recv_sem=c_rs.at[k, mask, part],
            device_id={"dp": peer[1 << bit]}, device_id_type=MESH)

    def rows_copy(k, mask):
        start = pl.multiple_of(peer[mask] * block, block)
        return pltpu.make_async_remote_copy(
            src_ref=rx.at[k, :, pl.ds(start, block)],
            dst_ref=xg.at[k, place(mask)],
            send_sem=g_ss.at[k, mask], recv_sem=g_rs.at[k, mask],
            device_id={"dp": peer[mask]}, device_id_type=MESH)

    waited = set()

    def arrive(k, mask, part):
        if mask and (k, mask, part) not in waited:
            waited.add((k, mask, part))
            delta_copy(k, mask, part).wait_recv()

    def pass_on(k, level):
        for mask in masks:
            if bin(mask).count("1") != level:
                continue
            for part in range(2):
                arrive(k, mask ^ (1 << via[mask, part]), part)
                copy = delta_copy(k, mask, part)
                copy.start()
                pending.append(copy)

    def compute(k):
        if k:
            x_copy[k].wait_recv()
        for mask in masks[::-1]:
            copy = rows_copy(k, mask)
            copy.start()
            pending.append(copy)
        if k == 0:
            load_g.wait()
            load_u.wait()
        else:
            d_copy[k].wait_recv()

        def forward(f, carry):
            cols = pl.ds(pl.multiple_of(f * tile, tile), tile)
            ucols = pl.ds(pl.multiple_of(f * tile + hidden, tile), tile)
            x = rx[k]
            gate = dot(x, wg[:, cols], 1, 0)
            up = dot(x, wu[:, cols], 1, 0)
            sig = jax.nn.sigmoid(gate)
            grad = rd[k, :, cols].astype(F32)
            dg[k, 0:cap, cols] = (grad * up * sig * (1.0 + gate * (1.0 - sig))).astype(BF)
            dg[k, 0:cap, ucols] = (grad * gate * sig).astype(BF)
            return carry

        lax.fori_loop(0, hidden // tile, forward, 0)
        pass_on(k, 1)
        held = sback if k else ret

        def backward(d, carry):
            cols = pl.ds(pl.multiple_of(d * tile, tile), tile)
            held[k, :, cols] = (
                dot(dg[k, 0:cap, 0:hidden], wg[cols, :], 1, 1)
                + dot(dg[k, 0:cap, hidden:], wu[cols, :], 1, 1)
            ).astype(BF)
            return carry

        lax.fori_loop(0, features // tile, backward, 0)
        if k:
            b_copy[k] = to_expert(sback, ret, b_ss, b_rs, k)
            b_copy[k].start()
            pending.append(b_copy[k])
        start = pl.multiple_of(dp * block, block)
        xg[k, 0:cap, :] = rx[k, :, pl.ds(start, block)]

    def weight(k):
        for mask in masks:
            rows_copy(k, mask).wait_recv()
            for part in range(2):
                arrive(k, mask, part)
        for part in range(2):
            value = dot(xg[k], dg[k, :, part * hidden : (part + 1) * hidden], 0, 0)
            if k == 0:
                acc[part] = value
            elif k < groups - 1:
                acc[part] += value
            else:
                (out_gate, out_up)[part][...] = acc[part] + value

    for k in range(groups):
        compute(k)
        for level in range(bits, 2, -1):
            if k - level + 2 >= 0:
                pass_on(k - level + 2, level)
        pass_on(k, 2)
        if k >= bits:
            weight(k - bits)
    for k in range(groups, groups + bits - 2):
        for level in range(bits, 2, -1):
            if 0 <= k - level + 2 < groups:
                pass_on(k - level + 2, level)
    for k in range(max(groups - bits, 0), groups - 1):
        weight(k)

    for k in range(1, groups):
        b_copy[k].wait_recv()
    for c in range(0, features, step):
        total = dot(pick[span(partner[0]), :], ret[0, :, c : c + step], 0, 0)
        for k in range(1, groups):
            total = total + dot(pick[span(partner[k]), :], ret[k, :, c : c + step], 0, 0)
        out_tok[:, c : c + step] = total.astype(BF)
    weight(groups - 1)

    for copy in pending:
        copy.wait_send()


def per_device(tokens, routes, grad_hidden, w_gate, w_up):
    tok_rows, features = tokens.shape
    per_token = routes.shape[1]
    hidden = w_gate.shape[2]
    groups = lax.axis_size("expert")
    ways = lax.axis_size("dp")
    pair_count = tok_rows * per_token
    cold_most = pair_count // groups
    cold_floor = cold_most - 2 - cold_most // 8
    hot_total = pair_count - (groups - 3) * cold_floor - cold_most
    hot_most = (hot_total + 1) // 2 + min((hot_total - 2 * cold_most - 2) // 2, cold_most // 4)
    cap = (max(hot_most, cold_most) + 15) // 16 * 16
    slots = groups * cap
    block = features // ways
    bits = ways.bit_length() - 1
    hops = len(rs_plan(bits)[1])
    half = ways // 2
    vmem = pl.BlockSpec(memory_space=pltpu.VMEM)
    hbm = pl.BlockSpec(memory_space=pl.ANY)
    dma = pltpu.SemaphoreType.DMA
    held = 2 * (
        2 * features * hidden + 3 * slots * tok_rows + 2 * slots * (2 * features + hidden)
        + ways * slots * (2 * hidden + block) + 2 * tok_rows * (features + hidden)
    ) + 4 * 4 * block * hidden
    if groups & (groups - 1) == 0 and bits >= 2 and held < 3 * (1 << 24):
        tok_grad, gate_grad, up_grad = pl.pallas_call(
            functools.partial(gather_kernel, groups, ways, cap),
            out_shape=(
                jax.ShapeDtypeStruct((tok_rows, features), BF),
                jax.ShapeDtypeStruct((block, hidden), F32),
                jax.ShapeDtypeStruct((block, hidden), F32),
            ),
            in_specs=[vmem, vmem, vmem, vmem, hbm, hbm],
            out_specs=(vmem, vmem, vmem),
            scratch_shapes=[
                pltpu.VMEM((features, hidden), BF),
                pltpu.VMEM((features, hidden), BF),
                pltpu.VMEM((slots, tok_rows), BF),
                pltpu.VMEM((slots, tok_rows), BF),
                pltpu.VMEM((slots, tok_rows), BF),
                pltpu.VMEM((groups, cap, features), BF),
                pltpu.VMEM((groups, cap, hidden), BF),
                pltpu.VMEM((groups, cap, features), BF),
                pltpu.VMEM((groups, cap, hidden), BF),
                pltpu.VMEM((groups, ways * cap, 2 * hidden), BF),
                pltpu.VMEM((groups, ways * cap, block), BF),
                pltpu.VMEM((groups, cap, features), BF),
                pltpu.VMEM((groups, cap, features), BF),
                pltpu.VMEM((2, block, hidden), F32),
                dma((2,)),
                dma((groups,)),
                dma((groups,)),
                dma((groups,)),
                dma((groups,)),
                dma((groups,)),
                dma((groups,)),
                dma((groups, ways)),
                dma((groups, ways)),
                dma((groups, ways, 2)),
                dma((groups, ways, 2)),
            ],
            compiler_params=pltpu.CompilerParams(collective_id=0, has_side_effects=True),
        )(tokens, routes.T, grad_hidden[:, 0], grad_hidden[:, 1], w_gate[0], w_up[0])
        return tok_grad, gate_grad[None], up_grad[None]
    tok_grad, gate_grad, up_grad = pl.pallas_call(
        functools.partial(kernel, groups, ways, cap),
        out_shape=(
            jax.ShapeDtypeStruct((tok_rows, features), BF),
            jax.ShapeDtypeStruct((block, hidden), F32),
            jax.ShapeDtypeStruct((block, hidden), F32),
        ),
        in_specs=[vmem, vmem, vmem, vmem, hbm, hbm],
        out_specs=(vmem, vmem, vmem),
        scratch_shapes=[
            pltpu.VMEM((features, hidden), BF),
            pltpu.VMEM((features, hidden), BF),
            pltpu.VMEM((slots, tok_rows), BF),
            pltpu.VMEM((slots, features + hidden), BF),
            pltpu.VMEM((slots, features + hidden), BF),
            pltpu.VMEM((slots, 2 * hidden), BF),
            pltpu.VMEM((slots, features), BF),
            pltpu.VMEM((slots, features), BF),
            pltpu.VMEM((half, block, 2 * hidden), BF),
            pltpu.VMEM((half, block, 2 * hidden), BF),
            pltpu.VMEM((hops, block, hidden), BF),
            pltpu.VMEM((hops, block, hidden), BF),
            pltpu.VMEM((2, half, block, hidden), F32),
            dma((2,)),
            dma((groups,)),
            dma((groups,)),
            dma((groups,)),
            dma((groups,)),
            dma((half,)),
            dma((half,)),
            dma((hops,)),
            dma((hops,)),
        ],
        compiler_params=pltpu.CompilerParams(collective_id=0, has_side_effects=True),
    )(tokens, routes.T, grad_hidden[:, 0], grad_hidden[:, 1], w_gate[0], w_up[0])
    return tok_grad, gate_grad[None], up_grad[None]


def solution(mesh):
    placed = (
        P(("dp", "expert"), None),
        P(("dp", "expert"), None),
        P(("dp", "expert"), None, None),
        P("expert", None, None),
        P("expert", None, None),
    )
    return jax.shard_map(
        per_device,
        mesh=mesh,
        in_specs=placed,
        out_specs=(P(("dp", "expert"), None), P("expert", "dp", None), P("expert", "dp", None)),
        check_vma=False,
    )
```

```python
import functools

import jax
import jax.numpy as jnp
from jax import lax
from jax.experimental import pallas as pl
from jax.experimental.pallas import tpu as pltpu
from jax.sharding import PartitionSpec as P

MESH = pl.DeviceIdType.MESH
BF = jnp.bfloat16
F32 = jnp.float32


def dot(a, b, da, db):
    return lax.dot_general(a, b, (((da,), (db,)), ((), ())), preferred_element_type=F32)


def rs_plan(bits):
    orders = (tuple(range(bits)), (0,) + tuple(range(bits - 1, 0, -1)))
    index = {}
    for which, order in enumerate(orders):
        done = 1
        for bit in order[1:]:
            flag = 1 << bit
            for mask in range(1 << bits):
                if mask & done or mask & flag:
                    continue
                index[which, bit, mask] = len(index)
            done |= flag
    return orders, index


def kernel(
    groups, ways, cap, tok_ref, rt_ref, gh0_ref, gh1_ref, wg_hbm, wu_hbm,
    out_tok, out_gate, out_up,
    wg, wu, pick, send, rows, delta, back, ret, core_send, core_recv, hop_send, hop_recv, acc,
    w_sem, z_ssem, z_rsem, b_ssem, b_rsem, c_ssem, c_rsem, h_ssem, h_rsem,
):
    features = tok_ref.shape[1]
    toks = tok_ref.shape[0]
    hidden = gh0_ref.shape[1]
    block = features // ways
    bits = ways.bit_length() - 1
    orders, index = rs_plan(bits)
    me = lax.axis_index("expert")
    dp = lax.axis_index("dp")
    my_bits = [lax.rem(dp // (1 << b), 2) for b in range(bits)]

    def peer_dp(mask):
        total = 0
        for b in range(bits):
            bit = 1 - my_bits[b] if mask >> b & 1 else my_bits[b]
            total = total + bit * (1 << b)
        return total

    load_g = pltpu.make_async_copy(wg_hbm, wg, w_sem.at[0])
    load_u = pltpu.make_async_copy(wu_hbm, wu, w_sem.at[1])
    load_g.start()
    load_u.start()

    barrier = pltpu.get_barrier_semaphore()
    for off in range(1, groups):
        pl.semaphore_signal(
            barrier, inc=1, device_id={"expert": lax.rem(me + off, groups)}, device_id_type=MESH
        )
    for b in range(bits):
        pl.semaphore_signal(
            barrier, inc=1, device_id={"dp": peer_dp(1 << b)}, device_id_type=MESH
        )

    r0 = rt_ref[0:1, :]
    r1 = rt_ref[1:2, :]
    wide = max(groups, 8)
    ids = lax.broadcasted_iota(jnp.int32, (wide, toks), 0)
    is0 = (ids == r0).astype(F32)
    is1 = (ids == r1).astype(F32)
    before = (
        lax.broadcasted_iota(jnp.int32, (toks, toks), 0)
        < lax.broadcasted_iota(jnp.int32, (toks, toks), 1)
    ).astype(F32).astype(BF)
    earlier = dot((is0 + is1).astype(BF), before, 1, 0)
    pos0 = r0.astype(F32) * cap + jnp.sum(is0 * earlier, axis=0, keepdims=True)
    pos1 = r1.astype(F32) * cap + jnp.sum(is1 * earlier, axis=0, keepdims=True)
    slot = lax.broadcasted_iota(jnp.int32, (groups * cap, toks), 0).astype(F32)
    m0 = (slot == pos0).astype(F32)
    m1 = (slot == pos1).astype(F32)
    pick[...] = (m0 + m1).astype(BF)
    send[:, features:] = (
        dot(m0.astype(BF), gh0_ref[...], 1, 0) + dot(m1.astype(BF), gh1_ref[...], 1, 0)
    ).astype(BF)
    step = 512
    for c in range(0, features, step):
        send[:, c : c + step] = dot(pick[...], tok_ref[:, c : c + step], 1, 0).astype(BF)

    pl.semaphore_wait(barrier, groups - 1 + bits)

    def span(i):
        return pl.ds(pl.multiple_of(i * cap, cap), cap)

    def exchange(src, dst, ssem, rsem):
        sends, recvs = [], []
        for off in range(1, groups):
            to = lax.rem(me + off, groups)
            frm = lax.rem(me + groups - off, groups)
            sends.append(pltpu.make_async_remote_copy(
                src_ref=src.at[span(to)], dst_ref=dst.at[span(me)],
                send_sem=ssem.at[off], recv_sem=rsem.at[off],
                device_id={"expert": to}, device_id_type=MESH))
            recvs.append(pltpu.make_async_remote_copy(
                src_ref=src.at[span(frm)], dst_ref=dst.at[span(frm)],
                send_sem=ssem.at[off], recv_sem=rsem.at[off],
                device_id={"expert": frm}, device_id_type=MESH))
        for copy in sends:
            copy.start()
        return sends, recvs

    out_sends, out_recvs = exchange(send, rows, z_ssem, z_rsem)
    rows[span(me), :] = send[span(me), :]
    load_g.wait()
    load_u.wait()
    for copy in out_recvs:
        copy.wait_recv()

    tile = 256

    def forward(f, carry):
        cols = pl.ds(pl.multiple_of(f * tile, tile), tile)
        ucols = pl.ds(pl.multiple_of(f * tile + hidden, tile), tile)
        dcols = pl.ds(pl.multiple_of(f * tile + features, tile), tile)
        x = rows[:, 0:features]
        gate = dot(x, wg[:, cols], 1, 0)
        up = dot(x, wu[:, cols], 1, 0)
        sig = jax.nn.sigmoid(gate)
        grad = rows[:, dcols].astype(F32)
        delta[:, cols] = (grad * up * sig * (1.0 + gate * (1.0 - sig))).astype(BF)
        delta[:, ucols] = (grad * gate * sig).astype(BF)
        return carry

    lax.fori_loop(0, hidden // tile, forward, 0)

    def weight_block(mask):
        start = pl.multiple_of(peer_dp(mask) * block, block)
        return dot(rows[:, pl.ds(start, block)], delta[...], 0, 0)

    core_sends = {}
    for mask in range(ways - 1, 0, -2):
        place = mask >> 1
        core_send[place] = weight_block(mask).astype(BF)
        copy = pltpu.make_async_remote_copy(
            src_ref=core_send.at[place], dst_ref=core_recv.at[place],
            send_sem=c_ssem.at[place], recv_sem=c_rsem.at[place],
            device_id={"dp": peer_dp(1)}, device_id_type=MESH)
        copy.start()
        core_sends[place] = copy

    def backward(d, carry):
        cols = pl.ds(pl.multiple_of(d * tile, tile), tile)
        back[:, cols] = (
            dot(delta[:, 0:hidden], wg[cols, :], 1, 1)
            + dot(delta[:, hidden:], wu[cols, :], 1, 1)
        ).astype(BF)
        return carry

    lax.fori_loop(0, features // tile, backward, 0)
    back_sends, back_recvs = exchange(back, ret, b_ssem, b_rsem)
    ret[span(me), :] = back[span(me), :]

    hop_sends = []

    def hop(which, bit, mask, value):
        at = index[which, bit, mask ^ (1 << bit)]
        hop_send[at] = value.astype(BF)
        copy = pltpu.make_async_remote_copy(
            src_ref=hop_send.at[at], dst_ref=hop_recv.at[at],
            send_sem=h_ssem.at[at], recv_sem=h_rsem.at[at],
            device_id={"dp": peer_dp(1 << bit)}, device_id_type=MESH)
        copy.start()
        hop_sends.append(copy)

    def arrived(which, bit, mask):
        at = index[which, bit, mask]
        pltpu.make_async_remote_copy(
            src_ref=hop_send.at[at], dst_ref=hop_recv.at[at],
            send_sem=h_ssem.at[at], recv_sem=h_rsem.at[at],
            device_id={"dp": peer_dp(1 << bit)}, device_id_type=MESH).wait_recv()
        return hop_recv[at].astype(F32)

    for mask in range(ways - 2, -1, -2):
        place = mask >> 1
        core_sends[place].wait_recv()
        total = weight_block(mask) + core_recv[place].astype(F32)
        for which in range(2):
            part = total[:, which * hidden : (which + 1) * hidden]
            bit = orders[which][1]
            if mask >> bit & 1:
                hop(which, bit, mask, part)
            else:
                acc[which, place] = part

    for level in range(2, bits):
        for mask in range(ways - 2, -1, -2):
            for which in range(2):
                order = orders[which]
                fixed = sum(1 << b for b in order[:level])
                if mask & fixed:
                    continue
                value = acc[which, mask >> 1] + arrived(which, order[level - 1], mask)
                if mask >> order[level] & 1:
                    hop(which, order[level], mask, value)
                else:
                    acc[which, mask >> 1] = value

    for copy in back_recvs:
        copy.wait_recv()
    for c in range(0, features, step):
        out_tok[:, c : c + step] = dot(pick[...], ret[:, c : c + step], 0, 0).astype(BF)
    out_gate[...] = acc[0, 0] + arrived(0, orders[0][-1], 0)
    out_up[...] = acc[1, 0] + arrived(1, orders[1][-1], 0)

    for copy in out_sends + back_sends + list(core_sends.values()) + hop_sends:
        copy.wait_send()


def gather_plan(bits):
    if bits > 2:
        orders = (tuple(range(1, bits)) + (0,), tuple(range(bits - 1, 0, -1)) + (0,))
    else:
        orders = (tuple(range(bits - 1, -1, -1)),) * 2
    via = {}
    for part, order in enumerate(orders):
        for mask in range(1, 1 << bits):
            via[mask, part] = [b for b in order if mask >> b & 1][-1]
    masks = sorted(range(1, 1 << bits), key=lambda mask: (bin(mask).count("1"), mask))
    return masks, via


def fold_width(extra, width):
    return width // 2 + (extra - 8) * 128


def fold(extra, rows):
    width = rows.shape[1]
    parts = [jnp.concatenate([rows[0:8, : width // 2], rows[0:8, width // 2 :]], axis=0)]
    sub = lax.broadcasted_iota(jnp.int32, (16, 128), 0)
    for j in range(8, extra):
        total = jnp.zeros((16, 128), F32)
        for c in range(width // 128):
            total = jnp.where(sub == c, rows[j : j + 1, c * 128 : (c + 1) * 128], total)
        parts.append(total)
    return jnp.concatenate([p.astype(BF) for p in parts], axis=1)


def unfold(extra, folded, width):
    rows = folded.astype(F32)
    top = jnp.concatenate([rows[0:8, : width // 2], rows[8:16, : width // 2]], axis=1)
    sub = lax.broadcasted_iota(jnp.int32, (8, width), 0)
    low = jnp.zeros((8, width), F32)
    for j in range(8, extra):
        at = width // 2 + (j - 8) * 128
        row = jnp.concatenate(
            [rows[c : c + 1, at : at + 128] for c in range(width // 128)], axis=1)
        low = jnp.where(sub == j - 8, row, low)
    return jnp.concatenate([top, low], axis=0).astype(BF)


def gather_kernel(
    groups, ways, cap, base, extra, rt_hbm, tok_hbm, gh_hbm, wg_hbm, wu_hbm,
    out_tok, out_gate, out_up,
    rt_ref, tok_ref, gh_ref, wg, wu, pick, both, sides, sx, sd, so, rx, rd, ro, dg, xg, sback, sbo, ret, rbo, acc,
    l_sem, x_ss, x_rs, d_ss, d_rs, o_ss, o_rs, b_ss, b_rs, e_ss, e_rs, g_ss, g_rs, c_ss, c_rs,
):
    toks, features = tok_ref.shape
    hidden = gh_ref.shape[2]
    wide_x = fold_width(extra, features)
    block = features // ways
    bits = ways.bit_length() - 1
    masks, via = gather_plan(bits)
    me = lax.axis_index("expert")
    dp = lax.axis_index("dp")

    def flip(value, mask, count):
        total = 0
        for b in range(count):
            bit = lax.rem(value // (1 << b), 2)
            if mask >> b & 1:
                bit = 1 - bit
            total = total + bit * (1 << b)
        return total

    partner = [flip(me, k, groups.bit_length() - 1) for k in range(groups)]
    peer = [flip(dp, m, bits) for m in range(ways)]

    load_r = pltpu.make_async_copy(rt_hbm, rt_ref, l_sem.at[4])
    load_r.start()
    load_t = pltpu.make_async_copy(tok_hbm, tok_ref, l_sem.at[0])
    load_d = pltpu.make_async_copy(gh_hbm, gh_ref, l_sem.at[1])
    load_g = pltpu.make_async_copy(wg_hbm, wg, l_sem.at[2])
    load_u = pltpu.make_async_copy(wu_hbm, wu, l_sem.at[3])
    load_t.start()
    load_d.start()
    load_g.start()
    load_u.start()

    barrier = pltpu.get_barrier_semaphore()
    for k in range(1, groups):
        pl.semaphore_signal(barrier, inc=1, device_id={"expert": partner[k]}, device_id_type=MESH)
    for m in range(1, ways):
        pl.semaphore_signal(barrier, inc=1, device_id={"dp": peer[m]}, device_id_type=MESH)

    load_r.wait()
    r0 = rt_ref[0:1, :]
    r1 = rt_ref[1:2, :]
    wide = max(groups, 8)
    ids = lax.broadcasted_iota(jnp.int32, (wide, toks), 0)
    is0 = (ids == r0).astype(F32)
    is1 = (ids == r1).astype(F32)
    before = (
        lax.broadcasted_iota(jnp.int32, (toks, toks), 0)
        < lax.broadcasted_iota(jnp.int32, (toks, toks), 1)
    ).astype(F32).astype(BF)
    earlier = dot((is0 + is1).astype(BF), before, 1, 0)
    pos0 = r0.astype(F32) * cap + jnp.sum(is0 * earlier, axis=0, keepdims=True)
    pos1 = r1.astype(F32) * cap + jnp.sum(is1 * earlier, axis=0, keepdims=True)
    slot = lax.broadcasted_iota(jnp.int32, (groups * cap, toks), 0).astype(F32)
    m0 = (slot == pos0).astype(F32)
    m1 = (slot == pos1).astype(F32)
    pick[...] = (m0 + m1).astype(BF)
    both[:, 0:toks] = m0.astype(BF)
    both[:, toks:] = m1.astype(BF)

    def rows_of(k, start, count):
        return pl.ds(pl.multiple_of(partner[k] * cap + start, 16), count)

    def to_expert(src, dst, ssem, rsem, k):
        return pltpu.make_async_remote_copy(
            src_ref=src.at[k, pl.ds(0, base)], dst_ref=dst.at[k, pl.ds(0, base)],
            send_sem=ssem.at[k], recv_sem=rsem.at[k],
            device_id={"expert": partner[k]}, device_id_type=MESH)

    def rest_to_expert(src, dst, ssem, rsem, k):
        return pltpu.make_async_remote_copy(
            src_ref=src.at[k], dst_ref=dst.at[k], send_sem=ssem.at[k], recv_sem=rsem.at[k],
            device_id={"expert": partner[k]}, device_id_type=MESH)

    pending = []
    x_copy, d_copy, o_copy, b_copy, e_copy = {}, {}, {}, {}, {}
    step = 512
    sequence = [0, 1] + list(range(groups - 1, 1, -1))
    load_t.wait()
    greeted = False
    for k in sequence[1:] + [0]:
        dest, count = (sx, base) if k else (rx, cap)
        for c in range(0, features, step):
            dest[k, 0:count, c : c + step] = dot(
                pick[rows_of(k, 0, count), :], tok_ref[:, c : c + step], 1, 0).astype(BF)
        if not greeted:
            with jax.named_scope("p_barrier"):
                pl.semaphore_wait(barrier, groups - 1 + ways - 1)
        if k:
            x_copy[k] = to_expert(sx, rx, x_ss, x_rs, k)
            x_copy[k].start()
            pending.append(x_copy[k])
        if not greeted:
            greeted = True
            load_d.wait()
            sides[0:toks, :] = gh_ref[:, 0, :]
            sides[toks:, :] = gh_ref[:, 1, :]
        dest = sd if k else rd
        dest[k, 0:count, :] = dot(both[rows_of(k, 0, count), :], sides[...], 1, 0).astype(BF)
        if k:
            d_copy[k] = to_expert(sd, rd, d_ss, d_rs, k)
            d_copy[k].start()
            over = rows_of(k, base, cap - base)
            so[k, :, 0:wide_x] = fold(extra, dot(pick[over, :], tok_ref[...], 1, 0))
            so[k, :, wide_x:] = fold(extra, dot(both[over, :], sides[...], 1, 0))
            o_copy[k] = rest_to_expert(so, ro, o_ss, o_rs, k)
            o_copy[k].start()
            pending += [d_copy[k], o_copy[k]]

    tile = 256

    def place(mask):
        return pl.ds(mask * cap, cap)

    def part_cols(part):
        return pl.ds(part * hidden, hidden)

    def delta_copy(k, mask, part):
        bit = via[mask, part]
        return pltpu.make_async_remote_copy(
            src_ref=dg.at[k, place(mask ^ (1 << bit)), part_cols(part)],
            dst_ref=dg.at[k, place(mask), part_cols(part)],
            send_sem=c_ss.at[k, mask, part], recv_sem=c_rs.at[k, mask, part],
            device_id={"dp": peer[1 << bit]}, device_id_type=MESH)

    def rows_copy(k, mask):
        start = pl.multiple_of(peer[mask] * block, block)
        return pltpu.make_async_remote_copy(
            src_ref=rx.at[k, :, pl.ds(start, block)],
            dst_ref=xg.at[k, place(mask)],
            send_sem=g_ss.at[k, mask], recv_sem=g_rs.at[k, mask],
            device_id={"dp": peer[mask]}, device_id_type=MESH)

    waited = set()

    def arrive(k, mask, part):
        if mask and (k, mask, part) not in waited:
            waited.add((k, mask, part))
            delta_copy(k, mask, part).wait_recv()

    def pass_on(k, level):
        steps = [(m, part) for part in range(2) for m in masks if bin(m).count("1") == level]
        steps.sort(key=lambda step: (via[step] == 0, step[1] != step[0] // (ways // 2)))
        for mask, part in steps:
            arrive(k, mask ^ (1 << via[mask, part]), part)
            copy = delta_copy(k, mask, part)
            copy.start()
            pending.append(copy)

    def compute(k):
        if k:
            with jax.named_scope(f"p_x{k}"):
                x_copy[k].wait_recv()
            with jax.named_scope(f"p_d{k}"):
                d_copy[k].wait_recv()
                o_copy[k].wait_recv()
            rx[k, base:cap, :] = unfold(extra, ro[k, :, 0:wide_x], features)
            rd[k, base:cap, :] = unfold(extra, ro[k, :, wide_x:], hidden)
        for mask in masks[::-1]:
            copy = rows_copy(k, mask)
            copy.start()
            pending.append(copy)
        if k == 0:
            load_g.wait()
            load_u.wait()

        def forward(f, carry):
            cols = pl.ds(pl.multiple_of(f * tile, tile), tile)
            ucols = pl.ds(pl.multiple_of(f * tile + hidden, tile), tile)
            x = rx[k]
            gate = dot(x, wg[:, cols], 1, 0)
            up = dot(x, wu[:, cols], 1, 0)
            sig = jax.nn.sigmoid(gate)
            grad = rd[k, :, cols].astype(F32)
            dg[k, 0:cap, cols] = (grad * up * sig * (1.0 + gate * (1.0 - sig))).astype(BF)
            dg[k, 0:cap, ucols] = (grad * gate * sig).astype(BF)
            return carry

        with jax.named_scope(f"p_fwd{k}"):
            lax.fori_loop(0, hidden // tile, forward, 0)
        pass_on(k, 1)
        held = sback if k else ret

        def backward(d, carry):
            cols = pl.ds(pl.multiple_of(d * tile, tile), tile)
            held[k, :, cols] = (
                dot(dg[k, 0:cap, 0:hidden], wg[cols, :], 1, 1)
                + dot(dg[k, 0:cap, hidden:], wu[cols, :], 1, 1)
            ).astype(BF)
            return carry

        with jax.named_scope(f"p_back{k}"):
            lax.fori_loop(0, features // tile, backward, 0)
        if k:
            b_copy[k] = to_expert(sback, ret, b_ss, b_rs, k)
            b_copy[k].start()
            sbo[k] = fold(extra, sback[k, base:cap, :].astype(F32))
            e_copy[k] = rest_to_expert(sbo, rbo, e_ss, e_rs, k)
            e_copy[k].start()
            pending.extend([b_copy[k], e_copy[k]])
        start = pl.multiple_of(dp * block, block)
        xg[k, 0:cap, :] = rx[k, :, pl.ds(start, block)]

    def weight(k):
        with jax.named_scope(f"p_got{k}"):
            for mask in masks:
                rows_copy(k, mask).wait_recv()
                for part in range(2):
                    arrive(k, mask, part)
        for part in range(2):
            value = dot(xg[k], dg[k, :, part * hidden : (part + 1) * hidden], 0, 0)
            if k == sequence[0]:
                acc[part] = value
            elif k != sequence[-1]:
                acc[part] += value
            else:
                (out_gate, out_up)[part][...] = acc[part] + value

    def hop(at, level):
        if 0 <= at < groups:
            with jax.named_scope(f"p_pass{sequence[at]}_{level}"):
                pass_on(sequence[at], level)

    for at in range(groups + bits):
        if at < groups:
            compute(sequence[at])
        for level in range(2, bits + 1):
            hop(at + 1 - level, level)
        if bits <= at < groups + bits - 1:
            weight(sequence[at - bits])

    for k in range(1, groups):
        with jax.named_scope(f"p_ret{k}"):
            b_copy[k].wait_recv()
            e_copy[k].wait_recv()
        ret[k, base:cap, :] = unfold(extra, rbo[k], features)
    for c in range(0, features, step):
        total = dot(pick[rows_of(0, 0, cap), :], ret[0, :, c : c + step], 0, 0)
        for k in range(1, groups):
            total = total + dot(pick[rows_of(k, 0, cap), :], ret[k, :, c : c + step], 0, 0)
        out_tok[:, c : c + step] = total.astype(BF)
    weight(sequence[-1])

    with jax.named_scope("p_drain"):
        for copy in pending:
            copy.wait_send()


def flush_kernel(tok, gate, up, out_tok, out_gate, out_up, sems):
    copies = [
        pltpu.make_async_copy(src, dst, sems.at[i])
        for i, (src, dst) in enumerate(((tok, out_tok), (gate, out_gate), (up, out_up)))
    ]
    for copy in copies:
        copy.start()
    for copy in copies:
        copy.wait()


def pin(array):
    return pltpu.with_memory_space_constraint(array, pltpu.HBM)


def per_device(tokens, routes, grad_hidden, w_gate, w_up):
    tok_rows, features = tokens.shape
    per_token = routes.shape[1]
    hidden = w_gate.shape[2]
    groups = lax.axis_size("expert")
    ways = lax.axis_size("dp")
    pair_count = tok_rows * per_token
    cold_most = pair_count // groups
    cold_floor = cold_most - 2 - cold_most // 8
    hot_total = pair_count - (groups - 3) * cold_floor - cold_most
    hot_most = (hot_total + 1) // 2 + min((hot_total - 2 * cold_most - 2) // 2, cold_most // 4)
    cap = (max(hot_most, cold_most) + 15) // 16 * 16
    slots = groups * cap
    block = features // ways
    bits = ways.bit_length() - 1
    hops = len(rs_plan(bits)[1])
    half = ways // 2
    vmem = pl.BlockSpec(memory_space=pltpu.VMEM)
    hbm = pl.BlockSpec(memory_space=pl.ANY)
    dma = pltpu.SemaphoreType.DMA
    base = max(hot_most, cold_most) // 16 * 16
    extra = max(hot_most, cold_most) - base
    held = 2 * (
        2 * features * hidden + 3 * slots * tok_rows + 5 * slots * (features + hidden)
        + ways * slots * (2 * hidden + block) + 2 * tok_rows * (features + 4 * hidden)
    ) + 4 * 4 * block * hidden
    if groups & (groups - 1) == 0 and bits >= 2 and 8 <= extra and features <= 2048 and held < 9 << 22:
        far = pl.BlockSpec(memory_space=pltpu.HBM)
        over = fold_width(extra, features)
        shapes = (
            jax.ShapeDtypeStruct((tok_rows, features), BF),
            jax.ShapeDtypeStruct((block, hidden), F32),
            jax.ShapeDtypeStruct((block, hidden), F32),
        )
        results = pl.pallas_call(
            functools.partial(gather_kernel, groups, ways, cap, base, extra),
            out_shape=shapes,
            in_specs=[far] * 5,
            out_specs=(vmem, vmem, vmem),
            scratch_shapes=[
                pltpu.VMEM((per_token, tok_rows), jnp.int32),
                pltpu.VMEM((tok_rows, features), BF),
                pltpu.VMEM((tok_rows, per_token, hidden), BF),
                pltpu.VMEM((features, hidden), BF),
                pltpu.VMEM((features, hidden), BF),
                pltpu.VMEM((slots, tok_rows), BF),
                pltpu.VMEM((slots, 2 * tok_rows), BF),
                pltpu.VMEM((2 * tok_rows, hidden), BF),
                pltpu.VMEM((groups, base, features), BF),
                pltpu.VMEM((groups, base, hidden), BF),
                pltpu.VMEM((groups, 16, over + fold_width(extra, hidden)), BF),
                pltpu.VMEM((groups, cap, features), BF),
                pltpu.VMEM((groups, cap, hidden), BF),
                pltpu.VMEM((groups, 16, over + fold_width(extra, hidden)), BF),
                pltpu.VMEM((groups, ways * cap, 2 * hidden), BF),
                pltpu.VMEM((groups, ways * cap, block), BF),
                pltpu.VMEM((groups, cap, features), BF),
                pltpu.VMEM((groups, 16, over), BF),
                pltpu.VMEM((groups, cap, features), BF),
                pltpu.VMEM((groups, 16, over), BF),
                pltpu.VMEM((2, block, hidden), F32),
                dma((5,)),
            ] + [dma((groups,))] * 10 + [dma((groups, ways))] * 2 + [dma((groups, ways, 2))] * 2,
            compiler_params=pltpu.CompilerParams(
                collective_id=0, has_side_effects=True, vmem_limit_bytes=10 << 22),
        )(pin(routes.T), pin(tokens), pin(grad_hidden), pin(w_gate[0]), pin(w_up[0]))
        tok_grad, gate_grad, up_grad = pl.pallas_call(
            flush_kernel,
            out_shape=shapes,
            in_specs=[vmem] * 3,
            out_specs=(far,) * 3,
            scratch_shapes=[dma((3,))],
            compiler_params=pltpu.CompilerParams(vmem_limit_bytes=1 << 20),
        )(*results)
        return tok_grad, gate_grad[None], up_grad[None]
    tok_grad, gate_grad, up_grad = pl.pallas_call(
        functools.partial(kernel, groups, ways, cap),
        out_shape=(
            jax.ShapeDtypeStruct((tok_rows, features), BF),
            jax.ShapeDtypeStruct((block, hidden), F32),
            jax.ShapeDtypeStruct((block, hidden), F32),
        ),
        in_specs=[vmem, vmem, vmem, vmem, hbm, hbm],
        out_specs=(vmem, vmem, vmem),
        scratch_shapes=[
            pltpu.VMEM((features, hidden), BF),
            pltpu.VMEM((features, hidden), BF),
            pltpu.VMEM((slots, tok_rows), BF),
            pltpu.VMEM((slots, features + hidden), BF),
            pltpu.VMEM((slots, features + hidden), BF),
            pltpu.VMEM((slots, 2 * hidden), BF),
            pltpu.VMEM((slots, features), BF),
            pltpu.VMEM((slots, features), BF),
            pltpu.VMEM((half, block, 2 * hidden), BF),
            pltpu.VMEM((half, block, 2 * hidden), BF),
            pltpu.VMEM((hops, block, hidden), BF),
            pltpu.VMEM((hops, block, hidden), BF),
            pltpu.VMEM((2, half, block, hidden), F32),
            dma((2,)),
            dma((groups,)),
            dma((groups,)),
            dma((groups,)),
            dma((groups,)),
            dma((half,)),
            dma((half,)),
            dma((hops,)),
            dma((hops,)),
        ],
        compiler_params=pltpu.CompilerParams(collective_id=0, has_side_effects=True),
    )(tokens, routes.T, grad_hidden[:, 0], grad_hidden[:, 1], w_gate[0], w_up[0])
    return tok_grad, gate_grad[None], up_grad[None]


def solution(mesh):
    placed = (
        P(("dp", "expert"), None),
        P(("dp", "expert"), None),
        P(("dp", "expert"), None, None),
        P("expert", None, None),
        P("expert", None, None),
    )
    return jax.shard_map(
        per_device,
        mesh=mesh,
        in_specs=placed,
        out_specs=(P(("dp", "expert"), None), P("expert", "dp", None), P("expert", "dp", None)),
        check_vma=False,
    )
```

```python
import functools

import jax
import jax.numpy as jnp
from jax import lax
from jax.experimental import pallas as pl
from jax.experimental.pallas import tpu as pltpu
from jax.sharding import PartitionSpec as P

MESH = pl.DeviceIdType.MESH
BF = jnp.bfloat16
F32 = jnp.float32


def dot(a, b, da, db):
    return lax.dot_general(a, b, (((da,), (db,)), ((), ())), preferred_element_type=F32)


def rs_plan(bits):
    orders = (tuple(range(bits)), (0,) + tuple(range(bits - 1, 0, -1)))
    index = {}
    for which, order in enumerate(orders):
        done = 1
        for bit in order[1:]:
            flag = 1 << bit
            for mask in range(1 << bits):
                if mask & done or mask & flag:
                    continue
                index[which, bit, mask] = len(index)
            done |= flag
    return orders, index


def kernel(
    groups, ways, cap, tok_ref, rt_ref, gh0_ref, gh1_ref, wg_hbm, wu_hbm,
    out_tok, out_gate, out_up,
    wg, wu, pick, send, rows, delta, back, ret, core_send, core_recv, hop_send, hop_recv, acc,
    w_sem, z_ssem, z_rsem, b_ssem, b_rsem, c_ssem, c_rsem, h_ssem, h_rsem,
):
    features = tok_ref.shape[1]
    toks = tok_ref.shape[0]
    hidden = gh0_ref.shape[1]
    block = features // ways
    bits = ways.bit_length() - 1
    orders, index = rs_plan(bits)
    me = lax.axis_index("expert")
    dp = lax.axis_index("dp")
    my_bits = [lax.rem(dp // (1 << b), 2) for b in range(bits)]

    def peer_dp(mask):
        total = 0
        for b in range(bits):
            bit = 1 - my_bits[b] if mask >> b & 1 else my_bits[b]
            total = total + bit * (1 << b)
        return total

    load_g = pltpu.make_async_copy(wg_hbm, wg, w_sem.at[0])
    load_u = pltpu.make_async_copy(wu_hbm, wu, w_sem.at[1])
    load_g.start()
    load_u.start()

    barrier = pltpu.get_barrier_semaphore()
    for off in range(1, groups):
        pl.semaphore_signal(
            barrier, inc=1, device_id={"expert": lax.rem(me + off, groups)}, device_id_type=MESH
        )
    for b in range(bits):
        pl.semaphore_signal(
            barrier, inc=1, device_id={"dp": peer_dp(1 << b)}, device_id_type=MESH
        )

    r0 = rt_ref[0:1, :]
    r1 = rt_ref[1:2, :]
    wide = max(groups, 8)
    ids = lax.broadcasted_iota(jnp.int32, (wide, toks), 0)
    is0 = (ids == r0).astype(F32)
    is1 = (ids == r1).astype(F32)
    before = (
        lax.broadcasted_iota(jnp.int32, (toks, toks), 0)
        < lax.broadcasted_iota(jnp.int32, (toks, toks), 1)
    ).astype(F32).astype(BF)
    earlier = dot((is0 + is1).astype(BF), before, 1, 0)
    pos0 = r0.astype(F32) * cap + jnp.sum(is0 * earlier, axis=0, keepdims=True)
    pos1 = r1.astype(F32) * cap + jnp.sum(is1 * earlier, axis=0, keepdims=True)
    slot = lax.broadcasted_iota(jnp.int32, (groups * cap, toks), 0).astype(F32)
    m0 = (slot == pos0).astype(F32)
    m1 = (slot == pos1).astype(F32)
    pick[...] = (m0 + m1).astype(BF)
    send[:, features:] = (
        dot(m0.astype(BF), gh0_ref[...], 1, 0) + dot(m1.astype(BF), gh1_ref[...], 1, 0)
    ).astype(BF)
    step = 512
    for c in range(0, features, step):
        send[:, c : c + step] = dot(pick[...], tok_ref[:, c : c + step], 1, 0).astype(BF)

    pl.semaphore_wait(barrier, groups - 1 + bits)

    def span(i):
        return pl.ds(pl.multiple_of(i * cap, cap), cap)

    def exchange(src, dst, ssem, rsem):
        sends, recvs = [], []
        for off in range(1, groups):
            to = lax.rem(me + off, groups)
            frm = lax.rem(me + groups - off, groups)
            sends.append(pltpu.make_async_remote_copy(
                src_ref=src.at[span(to)], dst_ref=dst.at[span(me)],
                send_sem=ssem.at[off], recv_sem=rsem.at[off],
                device_id={"expert": to}, device_id_type=MESH))
            recvs.append(pltpu.make_async_remote_copy(
                src_ref=src.at[span(frm)], dst_ref=dst.at[span(frm)],
                send_sem=ssem.at[off], recv_sem=rsem.at[off],
                device_id={"expert": frm}, device_id_type=MESH))
        for copy in sends:
            copy.start()
        return sends, recvs

    out_sends, out_recvs = exchange(send, rows, z_ssem, z_rsem)
    rows[span(me), :] = send[span(me), :]
    load_g.wait()
    load_u.wait()
    for copy in out_recvs:
        copy.wait_recv()

    tile = 256

    def forward(f, carry):
        cols = pl.ds(pl.multiple_of(f * tile, tile), tile)
        ucols = pl.ds(pl.multiple_of(f * tile + hidden, tile), tile)
        dcols = pl.ds(pl.multiple_of(f * tile + features, tile), tile)
        x = rows[:, 0:features]
        gate = dot(x, wg[:, cols], 1, 0)
        up = dot(x, wu[:, cols], 1, 0)
        sig = jax.nn.sigmoid(gate)
        grad = rows[:, dcols].astype(F32)
        delta[:, cols] = (grad * up * sig * (1.0 + gate * (1.0 - sig))).astype(BF)
        delta[:, ucols] = (grad * gate * sig).astype(BF)
        return carry

    lax.fori_loop(0, hidden // tile, forward, 0)

    def weight_block(mask):
        start = pl.multiple_of(peer_dp(mask) * block, block)
        return dot(rows[:, pl.ds(start, block)], delta[...], 0, 0)

    core_sends = {}
    for mask in range(ways - 1, 0, -2):
        place = mask >> 1
        core_send[place] = weight_block(mask).astype(BF)
        copy = pltpu.make_async_remote_copy(
            src_ref=core_send.at[place], dst_ref=core_recv.at[place],
            send_sem=c_ssem.at[place], recv_sem=c_rsem.at[place],
            device_id={"dp": peer_dp(1)}, device_id_type=MESH)
        copy.start()
        core_sends[place] = copy

    def backward(d, carry):
        cols = pl.ds(pl.multiple_of(d * tile, tile), tile)
        back[:, cols] = (
            dot(delta[:, 0:hidden], wg[cols, :], 1, 1)
            + dot(delta[:, hidden:], wu[cols, :], 1, 1)
        ).astype(BF)
        return carry

    lax.fori_loop(0, features // tile, backward, 0)
    back_sends, back_recvs = exchange(back, ret, b_ssem, b_rsem)
    ret[span(me), :] = back[span(me), :]

    hop_sends = []

    def hop(which, bit, mask, value):
        at = index[which, bit, mask ^ (1 << bit)]
        hop_send[at] = value.astype(BF)
        copy = pltpu.make_async_remote_copy(
            src_ref=hop_send.at[at], dst_ref=hop_recv.at[at],
            send_sem=h_ssem.at[at], recv_sem=h_rsem.at[at],
            device_id={"dp": peer_dp(1 << bit)}, device_id_type=MESH)
        copy.start()
        hop_sends.append(copy)

    def arrived(which, bit, mask):
        at = index[which, bit, mask]
        pltpu.make_async_remote_copy(
            src_ref=hop_send.at[at], dst_ref=hop_recv.at[at],
            send_sem=h_ssem.at[at], recv_sem=h_rsem.at[at],
            device_id={"dp": peer_dp(1 << bit)}, device_id_type=MESH).wait_recv()
        return hop_recv[at].astype(F32)

    for mask in range(ways - 2, -1, -2):
        place = mask >> 1
        core_sends[place].wait_recv()
        total = weight_block(mask) + core_recv[place].astype(F32)
        for which in range(2):
            part = total[:, which * hidden : (which + 1) * hidden]
            bit = orders[which][1]
            if mask >> bit & 1:
                hop(which, bit, mask, part)
            else:
                acc[which, place] = part

    for level in range(2, bits):
        for mask in range(ways - 2, -1, -2):
            for which in range(2):
                order = orders[which]
                fixed = sum(1 << b for b in order[:level])
                if mask & fixed:
                    continue
                value = acc[which, mask >> 1] + arrived(which, order[level - 1], mask)
                if mask >> order[level] & 1:
                    hop(which, order[level], mask, value)
                else:
                    acc[which, mask >> 1] = value

    for copy in back_recvs:
        copy.wait_recv()
    for c in range(0, features, step):
        out_tok[:, c : c + step] = dot(pick[...], ret[:, c : c + step], 0, 0).astype(BF)
    out_gate[...] = acc[0, 0] + arrived(0, orders[0][-1], 0)
    out_up[...] = acc[1, 0] + arrived(1, orders[1][-1], 0)

    for copy in out_sends + back_sends + list(core_sends.values()) + hop_sends:
        copy.wait_send()


def gather_plan(bits):
    if bits > 2:
        orders = (tuple(range(1, bits)) + (0,), tuple(range(bits - 1, 0, -1)) + (0,))
    else:
        orders = (tuple(range(bits - 1, -1, -1)),) * 2
    via = {}
    for part, order in enumerate(orders):
        for mask in range(1, 1 << bits):
            via[mask, part] = [b for b in order if mask >> b & 1][-1]
    masks = sorted(range(1, 1 << bits), key=lambda mask: (bin(mask).count("1"), mask))
    return masks, via


def fold_width(extra, width):
    return width // 2 + (extra - 8) * 128


def fold(extra, rows):
    width = rows.shape[1]
    parts = [jnp.concatenate([rows[0:8, : width // 2], rows[0:8, width // 2 :]], axis=0)]
    sub = lax.broadcasted_iota(jnp.int32, (16, 128), 0)
    for j in range(8, extra):
        total = jnp.zeros((16, 128), F32)
        for c in range(width // 128):
            total = jnp.where(sub == c, rows[j : j + 1, c * 128 : (c + 1) * 128], total)
        parts.append(total)
    return jnp.concatenate([p.astype(BF) for p in parts], axis=1)


def unfold(extra, folded, width):
    rows = folded.astype(F32)
    top = jnp.concatenate([rows[0:8, : width // 2], rows[8:16, : width // 2]], axis=1)
    sub = lax.broadcasted_iota(jnp.int32, (8, width), 0)
    low = jnp.zeros((8, width), F32)
    for j in range(8, extra):
        at = width // 2 + (j - 8) * 128
        row = jnp.concatenate(
            [rows[c : c + 1, at : at + 128] for c in range(width // 128)], axis=1)
        low = jnp.where(sub == j - 8, row, low)
    return jnp.concatenate([top, low], axis=0).astype(BF)


def gather_kernel(
    groups, ways, cap, base, extra, rt_hbm, tok_hbm, gh_hbm, wg_hbm, wu_hbm,
    out_tok, out_gate, out_up,
    rt_ref, tok_ref, gh_ref, wg, wu, pick, both, sides, sx, sd, so, rx, rd, ro, dg, xg, sback, sbo, ret, rbo, tot, acc,
    l_sem, z_ss, x_rs, d_rs, o_rs, b_rs, e_rs, g_ss, g_rs, c_ss, c_rs,
):
    toks, features = tok_ref.shape
    hidden = gh_ref.shape[2]
    wide_x = fold_width(extra, features)
    block = features // ways
    bits = ways.bit_length() - 1
    masks, via = gather_plan(bits)
    passed = sorted({(m ^ (1 << bit), part) for (m, part), bit in via.items()} - {(0, 0), (0, 1)})
    me = lax.axis_index("expert")
    dp = lax.axis_index("dp")

    def flip(value, mask, count):
        total = 0
        for b in range(count):
            bit = lax.rem(value // (1 << b), 2)
            if mask >> b & 1:
                bit = 1 - bit
            total = total + bit * (1 << b)
        return total

    partner = [flip(me, k, groups.bit_length() - 1) for k in range(groups)]
    peer = [flip(dp, m, bits) for m in range(ways)]

    load_r = pltpu.make_async_copy(rt_hbm, rt_ref, l_sem.at[4])
    load_r.start()
    load_t = pltpu.make_async_copy(tok_hbm, tok_ref, l_sem.at[0])
    load_d = pltpu.make_async_copy(gh_hbm, gh_ref, l_sem.at[1])
    load_g = pltpu.make_async_copy(wg_hbm, wg, l_sem.at[2])
    load_u = pltpu.make_async_copy(wu_hbm, wu, l_sem.at[3])
    load_t.start()
    load_d.start()
    load_g.start()
    load_u.start()

    barrier = pltpu.get_barrier_semaphore()
    for k in range(1, groups):
        pl.semaphore_signal(barrier, inc=1, device_id={"expert": partner[k]}, device_id_type=MESH)
    for m in range(1, ways):
        pl.semaphore_signal(barrier, inc=1, device_id={"dp": peer[m]}, device_id_type=MESH)

    load_r.wait()
    r0 = rt_ref[0:1, :]
    r1 = rt_ref[1:2, :]
    wide = max(groups, 8)
    ids = lax.broadcasted_iota(jnp.int32, (wide, toks), 0)
    is0 = (ids == r0).astype(F32)
    is1 = (ids == r1).astype(F32)
    before = (
        lax.broadcasted_iota(jnp.int32, (toks, toks), 0)
        < lax.broadcasted_iota(jnp.int32, (toks, toks), 1)
    ).astype(F32).astype(BF)
    earlier = dot((is0 + is1).astype(BF), before, 1, 0)
    pos0 = r0.astype(F32) * cap + jnp.sum(is0 * earlier, axis=0, keepdims=True)
    pos1 = r1.astype(F32) * cap + jnp.sum(is1 * earlier, axis=0, keepdims=True)
    slot = lax.broadcasted_iota(jnp.int32, (groups * cap, toks), 0).astype(F32)
    m0 = (slot == pos0).astype(F32)
    m1 = (slot == pos1).astype(F32)
    pick[...] = (m0 + m1).astype(BF)
    both[:, 0:toks] = m0.astype(BF)
    both[:, toks:] = m1.astype(BF)

    def rows_of(k, start, count):
        return pl.ds(pl.multiple_of(partner[k] * cap + start, 16), count)

    def to_expert(src, dst, kind, rsem, k):
        part = pl.ds(0, base if src.shape[1] >= base else src.shape[1])
        return pltpu.make_async_remote_copy(
            src_ref=src.at[k, part], dst_ref=dst.at[k, part],
            send_sem=z_ss.at[kind], recv_sem=rsem.at[k - 1],
            device_id={"expert": partner[k]}, device_id_type=MESH)

    def all_sent(ref, sem):
        pltpu.make_async_remote_copy(
            src_ref=ref, dst_ref=ref, send_sem=sem, recv_sem=sem,
            device_id={"dp": peer[1]}, device_id_type=MESH).wait_send()

    def all_got(ref, sem):
        pltpu.make_async_remote_copy(
            src_ref=ref, dst_ref=ref, send_sem=sem, recv_sem=sem,
            device_id={"dp": peer[1]}, device_id_type=MESH).wait_recv()

    x_copy, d_copy, o_copy = {}, {}, {}
    step = 512
    sequence = [0, 1] + list(range(groups - 1, 1, -1))
    load_t.wait()
    greeted = False
    for k in sequence[1:] + [0]:
        dest, count = (sx, base) if k else (rx, cap)
        for c in range(0, features, step):
            dest[k, 0:count, c : c + step] = dot(
                pick[rows_of(k, 0, count), :], tok_ref[:, c : c + step], 1, 0).astype(BF)
        if not greeted:
            with jax.named_scope("p_barrier"):
                pl.semaphore_wait(barrier, groups - 1 + ways - 1)
        if k:
            x_copy[k] = to_expert(sx, rx, 0, x_rs, k)
            x_copy[k].start()
        if not greeted:
            greeted = True
            load_d.wait()
            sides[0:toks, :] = gh_ref[:, 0, :]
            sides[toks:, :] = gh_ref[:, 1, :]
        dest = sd if k else rd
        dest[k, 0:count, :] = dot(both[rows_of(k, 0, count), :], sides[...], 1, 0).astype(BF)
        if k:
            d_copy[k] = to_expert(sd, rd, 1, d_rs, k)
            d_copy[k].start()
            over = rows_of(k, base, cap - base)
            so[k, :, 0:wide_x] = fold(extra, dot(pick[over, :], tok_ref[...], 1, 0))
            so[k, :, wide_x:] = fold(extra, dot(both[over, :], sides[...], 1, 0))
            o_copy[k] = to_expert(so, ro, 2, o_rs, k)
            o_copy[k].start()

    tile = 256

    def place(mask):
        return pl.ds(mask * cap, cap)

    def part_cols(part):
        return pl.ds(part * hidden, hidden)

    def delta_copy(k, mask, part):
        bit = via[mask, part]
        return pltpu.make_async_remote_copy(
            src_ref=dg.at[k, place(mask ^ (1 << bit)), part_cols(part)],
            dst_ref=dg.at[k, place(mask), part_cols(part)],
            send_sem=c_ss.at[0],
            recv_sem=c_rs.at[k, passed.index((mask, part)) if (mask, part) in passed else len(passed)],
            device_id={"dp": peer[1 << bit]}, device_id_type=MESH)

    def rows_copy(k, mask):
        start = pl.multiple_of(peer[mask] * block, block)
        return pltpu.make_async_remote_copy(
            src_ref=rx.at[k, :, pl.ds(start, block)],
            dst_ref=xg.at[k, place(mask)],
            send_sem=g_ss.at[0], recv_sem=g_rs.at[k],
            device_id={"dp": peer[mask]}, device_id_type=MESH)

    late = groups >= 4
    outer = lax.rem(me, 2) == me // (groups // 2)
    b_copy = {k: to_expert(sback, ret, 3, b_rs, k) for k in sequence[1:]}
    e_copy = {k: to_expert(sbo, rbo, 4, e_rs, k) for k in sequence[1:]}

    def give_back(k):
        b_copy[k].start()
        e_copy[k].start()

    waited = set()

    def arrive(k, mask, part):
        if mask and (k, mask, part) not in waited:
            waited.add((k, mask, part))
            delta_copy(k, mask, part).wait_recv()

    def pass_on(k, level):
        steps = [(m, part) for part in range(2) for m in masks if bin(m).count("1") == level]
        steps.sort(key=lambda step: (via[step] == 0, step[1] != step[0] // (ways // 2)))
        for mask, part in steps:
            arrive(k, mask ^ (1 << via[mask, part]), part)
            delta_copy(k, mask, part).start()

    def compute(k):
        if k:
            with jax.named_scope(f"p_x{k}"):
                x_copy[k].wait_recv()
            with jax.named_scope(f"p_d{k}"):
                d_copy[k].wait_recv()
                o_copy[k].wait_recv()
            if late and k == sequence[-1]:
                @pl.when(outer)
                def _():
                    give_back(sequence[-2])
            rx[k, base:cap, :] = unfold(extra, ro[k, :, 0:wide_x], features)
            rd[k, base:cap, :] = unfold(extra, ro[k, :, wide_x:], hidden)
        for mask in masks[::-1]:
            rows_copy(k, mask).start()
        if k == 0:
            load_g.wait()
            load_u.wait()

        def forward(f, carry):
            cols = pl.ds(pl.multiple_of(f * tile, tile), tile)
            ucols = pl.ds(pl.multiple_of(f * tile + hidden, tile), tile)
            x = rx[k]
            gate = dot(x, wg[:, cols], 1, 0)
            up = dot(x, wu[:, cols], 1, 0)
            sig = jax.nn.sigmoid(gate)
            grad = rd[k, :, cols].astype(F32)
            dg[k, 0:cap, cols] = (grad * up * sig * (1.0 + gate * (1.0 - sig))).astype(BF)
            dg[k, 0:cap, ucols] = (grad * gate * sig).astype(BF)
            return carry

        with jax.named_scope(f"p_fwd{k}"):
            lax.fori_loop(0, hidden // tile, forward, 0)
        pass_on(k, 1)
        held = sback if k else ret

        def backward(d, carry):
            cols = pl.ds(pl.multiple_of(d * tile, tile), tile)
            held[k, :, cols] = (
                dot(dg[k, 0:cap, 0:hidden], wg[cols, :], 1, 1)
                + dot(dg[k, 0:cap, hidden:], wu[cols, :], 1, 1)
            ).astype(BF)
            return carry

        with jax.named_scope(f"p_back{k}"):
            lax.fori_loop(0, features // tile, backward, 0)
        if k:
            sbo[k] = fold(extra, sback[k, base:cap, :].astype(F32))
            if not late or k != sequence[-2]:
                give_back(k)
            if late and k == sequence[-1]:
                @pl.when(jnp.logical_not(outer))
                def _():
                    give_back(sequence[-2])
        start = pl.multiple_of(dp * block, block)
        xg[k, 0:cap, :] = rx[k, :, pl.ds(start, block)]

    def weight(k):
        with jax.named_scope(f"p_got{k}"):
            all_got(xg.at[k, pl.ds(cap, (ways - 1) * cap)], g_rs.at[k])
            for mask, part in passed:
                arrive(k, mask, part)
            leaves = 2 * (ways - 1) - len(passed)
            all_got(dg.at[k, pl.ds(0, leaves * cap), part_cols(0)], c_rs.at[k, len(passed)])
        for part in range(2):
            value = dot(xg[k], dg[k, :, part * hidden : (part + 1) * hidden], 0, 0)
            if k == sequence[0]:
                acc[part] = value
            elif k != sequence[-1]:
                acc[part] += value
            else:
                (out_gate, out_up)[part][...] = acc[part] + value

    def hop(at, level):
        if 0 <= at < groups:
            with jax.named_scope(f"p_pass{sequence[at]}_{level}"):
                pass_on(sequence[at], level)

    for at in range(groups + bits):
        if at < groups:
            compute(sequence[at])
        for level in range(2, bits + 1):
            hop(at + 1 - level, level)
        if bits <= at < groups + bits - 1:
            weight(sequence[at - bits])
            if at == groups:
                for c in range(0, features, step):
                    tot[:, c : c + step] = dot(pick[rows_of(0, 0, cap), :], ret[0, :, c : c + step], 0, 0)
    weight(sequence[-1])

    for k in sequence[1:]:
        with jax.named_scope(f"p_ret{k}"):
            b_copy[k].wait_recv()
            e_copy[k].wait_recv()
        ret[k, base:cap, :] = unfold(extra, rbo[k], features)
        for c in range(0, features, step):
            total = tot[:, c : c + step] + dot(pick[rows_of(k, 0, cap), :], ret[k, :, c : c + step], 0, 0)
            if k == sequence[-1]:
                out_tok[:, c : c + step] = total.astype(BF)
            else:
                tot[:, c : c + step] = total

    with jax.named_scope("p_drain"):
        for kind, ref in enumerate((sx, sd, so, sx, sbo)):
            all_sent(ref.at[pl.ds(1, groups - 1)], z_ss.at[kind])
        all_sent(xg.at[pl.ds(0, groups), pl.ds(cap, (ways - 1) * cap)], g_ss.at[0])
        all_sent(dg.at[pl.ds(0, groups), pl.ds(cap, (ways - 1) * cap)], c_ss.at[0])


def flush_kernel(tok, gate, up, out_tok, out_gate, out_up, sems):
    copies = [
        pltpu.make_async_copy(src, dst, sems.at[i])
        for i, (src, dst) in enumerate(((tok, out_tok), (gate, out_gate), (up, out_up)))
    ]
    for copy in copies:
        copy.start()
    for copy in copies:
        copy.wait()


def pin(array):
    return pltpu.with_memory_space_constraint(array, pltpu.HBM)


def per_device(tokens, routes, grad_hidden, w_gate, w_up):
    tok_rows, features = tokens.shape
    per_token = routes.shape[1]
    hidden = w_gate.shape[2]
    groups = lax.axis_size("expert")
    ways = lax.axis_size("dp")
    pair_count = tok_rows * per_token
    cold_most = pair_count // groups
    cold_floor = cold_most - 2 - cold_most // 8
    hot_total = pair_count - (groups - 3) * cold_floor - cold_most
    hot_most = (hot_total + 1) // 2 + min((hot_total - 2 * cold_most - 2) // 2, cold_most // 4)
    cap = (max(hot_most, cold_most) + 15) // 16 * 16
    slots = groups * cap
    block = features // ways
    bits = ways.bit_length() - 1
    hops = len(rs_plan(bits)[1])
    half = ways // 2
    vmem = pl.BlockSpec(memory_space=pltpu.VMEM)
    hbm = pl.BlockSpec(memory_space=pl.ANY)
    dma = pltpu.SemaphoreType.DMA
    base = max(hot_most, cold_most) // 16 * 16
    extra = max(hot_most, cold_most) - base
    held = 2 * (
        2 * features * hidden + 3 * slots * tok_rows + 5 * slots * (features + hidden)
        + ways * slots * (2 * hidden + block) + 2 * tok_rows * (features + 4 * hidden)
    ) + 4 * 4 * block * hidden
    if groups & (groups - 1) == 0 and bits >= 2 and 8 <= extra and features <= 2048 and held < 9 << 22:
        far = pl.BlockSpec(memory_space=pltpu.HBM)
        over = fold_width(extra, features)
        shapes = (
            jax.ShapeDtypeStruct((tok_rows, features), BF),
            jax.ShapeDtypeStruct((block, hidden), F32),
            jax.ShapeDtypeStruct((block, hidden), F32),
        )
        results = pl.pallas_call(
            functools.partial(gather_kernel, groups, ways, cap, base, extra),
            out_shape=shapes,
            in_specs=[far] * 5,
            out_specs=(vmem, vmem, vmem),
            scratch_shapes=[
                pltpu.VMEM((per_token, tok_rows), jnp.int32),
                pltpu.VMEM((tok_rows, features), BF),
                pltpu.VMEM((tok_rows, per_token, hidden), BF),
                pltpu.VMEM((features, hidden), BF),
                pltpu.VMEM((features, hidden), BF),
                pltpu.VMEM((slots, tok_rows), BF),
                pltpu.VMEM((slots, 2 * tok_rows), BF),
                pltpu.VMEM((2 * tok_rows, hidden), BF),
                pltpu.VMEM((groups, base, features), BF),
                pltpu.VMEM((groups, base, hidden), BF),
                pltpu.VMEM((groups, 16, over + fold_width(extra, hidden)), BF),
                pltpu.VMEM((groups, cap, features), BF),
                pltpu.VMEM((groups, cap, hidden), BF),
                pltpu.VMEM((groups, 16, over + fold_width(extra, hidden)), BF),
                pltpu.VMEM((groups, ways * cap, 2 * hidden), BF),
                pltpu.VMEM((groups, ways * cap, block), BF),
                pltpu.VMEM((groups, cap, features), BF),
                pltpu.VMEM((groups, 16, over), BF),
                pltpu.VMEM((groups, cap, features), BF),
                pltpu.VMEM((groups, 16, over), BF),
                pltpu.VMEM((tok_rows, features), F32),
                pltpu.VMEM((2, block, hidden), F32),
                dma((5,)),
                dma((5,)),
            ] + [dma((groups - 1,))] * 5 + [dma((1,)), dma((groups,)), dma((1,)), dma((groups, ways - 1))],
            compiler_params=pltpu.CompilerParams(
                collective_id=0, has_side_effects=True, vmem_limit_bytes=10 << 22),
        )(pin(routes.T), pin(tokens), pin(grad_hidden), pin(w_gate[0]), pin(w_up[0]))
        tok_grad, gate_grad, up_grad = pl.pallas_call(
            flush_kernel,
            out_shape=shapes,
            in_specs=[vmem] * 3,
            out_specs=(far,) * 3,
            scratch_shapes=[dma((3,))],
            compiler_params=pltpu.CompilerParams(vmem_limit_bytes=1 << 20),
        )(*results)
        return tok_grad, gate_grad[None], up_grad[None]
    tok_grad, gate_grad, up_grad = pl.pallas_call(
        functools.partial(kernel, groups, ways, cap),
        out_shape=(
            jax.ShapeDtypeStruct((tok_rows, features), BF),
            jax.ShapeDtypeStruct((block, hidden), F32),
            jax.ShapeDtypeStruct((block, hidden), F32),
        ),
        in_specs=[vmem, vmem, vmem, vmem, hbm, hbm],
        out_specs=(vmem, vmem, vmem),
        scratch_shapes=[
            pltpu.VMEM((features, hidden), BF),
            pltpu.VMEM((features, hidden), BF),
            pltpu.VMEM((slots, tok_rows), BF),
            pltpu.VMEM((slots, features + hidden), BF),
            pltpu.VMEM((slots, features + hidden), BF),
            pltpu.VMEM((slots, 2 * hidden), BF),
            pltpu.VMEM((slots, features), BF),
            pltpu.VMEM((slots, features), BF),
            pltpu.VMEM((half, block, 2 * hidden), BF),
            pltpu.VMEM((half, block, 2 * hidden), BF),
            pltpu.VMEM((hops, block, hidden), BF),
            pltpu.VMEM((hops, block, hidden), BF),
            pltpu.VMEM((2, half, block, hidden), F32),
            dma((2,)),
            dma((groups,)),
            dma((groups,)),
            dma((groups,)),
            dma((groups,)),
            dma((half,)),
            dma((half,)),
            dma((hops,)),
            dma((hops,)),
        ],
        compiler_params=pltpu.CompilerParams(collective_id=0, has_side_effects=True),
    )(tokens, routes.T, grad_hidden[:, 0], grad_hidden[:, 1], w_gate[0], w_up[0])
    return tok_grad, gate_grad[None], up_grad[None]


def solution(mesh):
    placed = (
        P(("dp", "expert"), None),
        P(("dp", "expert"), None),
        P(("dp", "expert"), None, None),
        P("expert", None, None),
        P("expert", None, None),
    )
    return jax.shard_map(
        per_device,
        mesh=mesh,
        in_specs=placed,
        out_specs=(P(("dp", "expert"), None), P("expert", "dp", None), P("expert", "dp", None)),
        check_vma=False,
    )
```

```python
import functools

import jax
import jax.numpy as jnp
from jax import lax
from jax.experimental import pallas as pl
from jax.experimental.pallas import tpu as pltpu
from jax.sharding import PartitionSpec as P

MESH = pl.DeviceIdType.MESH
BF = jnp.bfloat16
F32 = jnp.float32


def dot(a, b, da, db):
    return lax.dot_general(a, b, (((da,), (db,)), ((), ())), preferred_element_type=F32)


def rs_plan(bits):
    orders = (tuple(range(bits)), (0,) + tuple(range(bits - 1, 0, -1)))
    index = {}
    for which, order in enumerate(orders):
        done = 1
        for bit in order[1:]:
            flag = 1 << bit
            for mask in range(1 << bits):
                if mask & done or mask & flag:
                    continue
                index[which, bit, mask] = len(index)
            done |= flag
    return orders, index


def kernel(
    groups, ways, cap, tok_ref, rt_ref, gh0_ref, gh1_ref, wg_hbm, wu_hbm,
    out_tok, out_gate, out_up,
    wg, wu, pick, send, rows, delta, back, ret, core_send, core_recv, hop_send, hop_recv, acc,
    w_sem, z_ssem, z_rsem, b_ssem, b_rsem, c_ssem, c_rsem, h_ssem, h_rsem,
):
    features = tok_ref.shape[1]
    toks = tok_ref.shape[0]
    hidden = gh0_ref.shape[1]
    block = features // ways
    bits = ways.bit_length() - 1
    orders, index = rs_plan(bits)
    me = lax.axis_index("expert")
    dp = lax.axis_index("dp")
    my_bits = [lax.rem(dp // (1 << b), 2) for b in range(bits)]

    def peer_dp(mask):
        total = 0
        for b in range(bits):
            bit = 1 - my_bits[b] if mask >> b & 1 else my_bits[b]
            total = total + bit * (1 << b)
        return total

    load_g = pltpu.make_async_copy(wg_hbm, wg, w_sem.at[0])
    load_u = pltpu.make_async_copy(wu_hbm, wu, w_sem.at[1])
    load_g.start()
    load_u.start()

    barrier = pltpu.get_barrier_semaphore()
    for off in range(1, groups):
        pl.semaphore_signal(
            barrier, inc=1, device_id={"expert": lax.rem(me + off, groups)}, device_id_type=MESH
        )
    for b in range(bits):
        pl.semaphore_signal(
            barrier, inc=1, device_id={"dp": peer_dp(1 << b)}, device_id_type=MESH
        )

    r0 = rt_ref[0:1, :]
    r1 = rt_ref[1:2, :]
    wide = max(groups, 8)
    ids = lax.broadcasted_iota(jnp.int32, (wide, toks), 0)
    is0 = (ids == r0).astype(F32)
    is1 = (ids == r1).astype(F32)
    before = (
        lax.broadcasted_iota(jnp.int32, (toks, toks), 0)
        < lax.broadcasted_iota(jnp.int32, (toks, toks), 1)
    ).astype(F32).astype(BF)
    earlier = dot((is0 + is1).astype(BF), before, 1, 0)
    pos0 = r0.astype(F32) * cap + jnp.sum(is0 * earlier, axis=0, keepdims=True)
    pos1 = r1.astype(F32) * cap + jnp.sum(is1 * earlier, axis=0, keepdims=True)
    slot = lax.broadcasted_iota(jnp.int32, (groups * cap, toks), 0).astype(F32)
    m0 = (slot == pos0).astype(F32)
    m1 = (slot == pos1).astype(F32)
    pick[...] = (m0 + m1).astype(BF)
    send[:, features:] = (
        dot(m0.astype(BF), gh0_ref[...], 1, 0) + dot(m1.astype(BF), gh1_ref[...], 1, 0)
    ).astype(BF)
    step = 512
    for c in range(0, features, step):
        send[:, c : c + step] = dot(pick[...], tok_ref[:, c : c + step], 1, 0).astype(BF)

    pl.semaphore_wait(barrier, groups - 1 + bits)

    def span(i):
        return pl.ds(pl.multiple_of(i * cap, cap), cap)

    def exchange(src, dst, ssem, rsem):
        sends, recvs = [], []
        for off in range(1, groups):
            to = lax.rem(me + off, groups)
            frm = lax.rem(me + groups - off, groups)
            sends.append(pltpu.make_async_remote_copy(
                src_ref=src.at[span(to)], dst_ref=dst.at[span(me)],
                send_sem=ssem.at[off], recv_sem=rsem.at[off],
                device_id={"expert": to}, device_id_type=MESH))
            recvs.append(pltpu.make_async_remote_copy(
                src_ref=src.at[span(frm)], dst_ref=dst.at[span(frm)],
                send_sem=ssem.at[off], recv_sem=rsem.at[off],
                device_id={"expert": frm}, device_id_type=MESH))
        for copy in sends:
            copy.start()
        return sends, recvs

    out_sends, out_recvs = exchange(send, rows, z_ssem, z_rsem)
    rows[span(me), :] = send[span(me), :]
    load_g.wait()
    load_u.wait()
    for copy in out_recvs:
        copy.wait_recv()

    tile = 256

    def forward(f, carry):
        cols = pl.ds(pl.multiple_of(f * tile, tile), tile)
        ucols = pl.ds(pl.multiple_of(f * tile + hidden, tile), tile)
        dcols = pl.ds(pl.multiple_of(f * tile + features, tile), tile)
        x = rows[:, 0:features]
        gate = dot(x, wg[:, cols], 1, 0)
        up = dot(x, wu[:, cols], 1, 0)
        sig = jax.nn.sigmoid(gate)
        grad = rows[:, dcols].astype(F32)
        delta[:, cols] = (grad * up * sig * (1.0 + gate * (1.0 - sig))).astype(BF)
        delta[:, ucols] = (grad * gate * sig).astype(BF)
        return carry

    lax.fori_loop(0, hidden // tile, forward, 0)

    def weight_block(mask):
        start = pl.multiple_of(peer_dp(mask) * block, block)
        return dot(rows[:, pl.ds(start, block)], delta[...], 0, 0)

    core_sends = {}
    for mask in range(ways - 1, 0, -2):
        place = mask >> 1
        core_send[place] = weight_block(mask).astype(BF)
        copy = pltpu.make_async_remote_copy(
            src_ref=core_send.at[place], dst_ref=core_recv.at[place],
            send_sem=c_ssem.at[place], recv_sem=c_rsem.at[place],
            device_id={"dp": peer_dp(1)}, device_id_type=MESH)
        copy.start()
        core_sends[place] = copy

    def backward(d, carry):
        cols = pl.ds(pl.multiple_of(d * tile, tile), tile)
        back[:, cols] = (
            dot(delta[:, 0:hidden], wg[cols, :], 1, 1)
            + dot(delta[:, hidden:], wu[cols, :], 1, 1)
        ).astype(BF)
        return carry

    lax.fori_loop(0, features // tile, backward, 0)
    back_sends, back_recvs = exchange(back, ret, b_ssem, b_rsem)
    ret[span(me), :] = back[span(me), :]

    hop_sends = []

    def hop(which, bit, mask, value):
        at = index[which, bit, mask ^ (1 << bit)]
        hop_send[at] = value.astype(BF)
        copy = pltpu.make_async_remote_copy(
            src_ref=hop_send.at[at], dst_ref=hop_recv.at[at],
            send_sem=h_ssem.at[at], recv_sem=h_rsem.at[at],
            device_id={"dp": peer_dp(1 << bit)}, device_id_type=MESH)
        copy.start()
        hop_sends.append(copy)

    def arrived(which, bit, mask):
        at = index[which, bit, mask]
        pltpu.make_async_remote_copy(
            src_ref=hop_send.at[at], dst_ref=hop_recv.at[at],
            send_sem=h_ssem.at[at], recv_sem=h_rsem.at[at],
            device_id={"dp": peer_dp(1 << bit)}, device_id_type=MESH).wait_recv()
        return hop_recv[at].astype(F32)

    for mask in range(ways - 2, -1, -2):
        place = mask >> 1
        core_sends[place].wait_recv()
        total = weight_block(mask) + core_recv[place].astype(F32)
        for which in range(2):
            part = total[:, which * hidden : (which + 1) * hidden]
            bit = orders[which][1]
            if mask >> bit & 1:
                hop(which, bit, mask, part)
            else:
                acc[which, place] = part

    for level in range(2, bits):
        for mask in range(ways - 2, -1, -2):
            for which in range(2):
                order = orders[which]
                fixed = sum(1 << b for b in order[:level])
                if mask & fixed:
                    continue
                value = acc[which, mask >> 1] + arrived(which, order[level - 1], mask)
                if mask >> order[level] & 1:
                    hop(which, order[level], mask, value)
                else:
                    acc[which, mask >> 1] = value

    for copy in back_recvs:
        copy.wait_recv()
    for c in range(0, features, step):
        out_tok[:, c : c + step] = dot(pick[...], ret[:, c : c + step], 0, 0).astype(BF)
    out_gate[...] = acc[0, 0] + arrived(0, orders[0][-1], 0)
    out_up[...] = acc[1, 0] + arrived(1, orders[1][-1], 0)

    for copy in out_sends + back_sends + list(core_sends.values()) + hop_sends:
        copy.wait_send()


def gather_plan(bits):
    if bits > 2:
        orders = (tuple(range(1, bits)) + (0,), tuple(range(bits - 1, 0, -1)) + (0,))
    else:
        orders = (tuple(range(bits - 1, -1, -1)),) * 2
    via = {}
    for part, order in enumerate(orders):
        for mask in range(1, 1 << bits):
            via[mask, part] = [b for b in order if mask >> b & 1][-1]
    masks = sorted(range(1, 1 << bits), key=lambda mask: (bin(mask).count("1"), mask))
    return masks, via


def fold_width(extra, width):
    return width // 2 + (extra - 8) * 128


def fold(extra, rows):
    width = rows.shape[1]
    parts = [jnp.concatenate([rows[0:8, : width // 2], rows[0:8, width // 2 :]], axis=0)]
    sub = lax.broadcasted_iota(jnp.int32, (16, 128), 0)
    for j in range(8, extra):
        total = jnp.zeros((16, 128), F32)
        for c in range(width // 128):
            total = jnp.where(sub == c, rows[j : j + 1, c * 128 : (c + 1) * 128], total)
        parts.append(total)
    return jnp.concatenate([p.astype(BF) for p in parts], axis=1)


def unfold(extra, folded, width):
    rows = folded.astype(F32)
    top = jnp.concatenate([rows[0:8, : width // 2], rows[8:16, : width // 2]], axis=1)
    sub = lax.broadcasted_iota(jnp.int32, (8, width), 0)
    low = jnp.zeros((8, width), F32)
    for j in range(8, extra):
        at = width // 2 + (j - 8) * 128
        row = jnp.concatenate(
            [rows[c : c + 1, at : at + 128] for c in range(width // 128)], axis=1)
        low = jnp.where(sub == j - 8, row, low)
    return jnp.concatenate([top, low], axis=0).astype(BF)


def gather_kernel(
    groups, ways, cap, base, extra, rt_hbm, tok_hbm, gh_hbm, wg_hbm, wu_hbm,
    out_tok, out_gate, out_up,
    rt_ref, tok_ref, gh_ref, wg, wu, pick, both, sides, sx, sd, so, rx, rd, ro, spos, fpos, far, pfar, rel, dg, xg, sback, sbo, ret, rbo, tot, acc,
    l_sem, f_ss, f_rs, p_rs, q_rs, z_ss, x_rs, d_rs, o_rs, b_rs, e_rs, g_ss, g_rs, c_ss, c_rs,
):
    toks, features = tok_ref.shape
    hidden = gh_ref.shape[2]
    wide_x = fold_width(extra, features)
    block = features // ways
    bits = ways.bit_length() - 1
    masks, via = gather_plan(bits)
    passed = sorted({(m ^ (1 << bit), part) for (m, part), bit in via.items()} - {(0, 0), (0, 1)})
    me = lax.axis_index("expert")
    dp = lax.axis_index("dp")

    def flip(value, mask, count):
        total = 0
        for b in range(count):
            bit = lax.rem(value // (1 << b), 2)
            if mask >> b & 1:
                bit = 1 - bit
            total = total + bit * (1 << b)
        return total

    partner = [flip(me, k, groups.bit_length() - 1) for k in range(groups)]
    peer = [flip(dp, m, bits) for m in range(ways)]

    load_r = pltpu.make_async_copy(rt_hbm, rt_ref, l_sem.at[4])
    load_r.start()
    load_t = pltpu.make_async_copy(tok_hbm, tok_ref, l_sem.at[0])
    load_d = pltpu.make_async_copy(gh_hbm, gh_ref, l_sem.at[1])
    load_g = pltpu.make_async_copy(wg_hbm, wg, l_sem.at[2])
    load_u = pltpu.make_async_copy(wu_hbm, wu, l_sem.at[3])
    load_t.start()
    load_d.start()
    load_g.start()
    load_u.start()

    barrier = pltpu.get_barrier_semaphore()
    for k in range(1, groups):
        pl.semaphore_signal(barrier, inc=1, device_id={"expert": partner[k]}, device_id_type=MESH)
    for m in range(1, ways):
        pl.semaphore_signal(barrier, inc=1, device_id={"dp": peer[m]}, device_id_type=MESH)

    load_r.wait()
    r0 = rt_ref[0:1, :]
    r1 = rt_ref[1:2, :]
    wide = max(groups, 8)
    ids = lax.broadcasted_iota(jnp.int32, (wide, toks), 0)
    is0 = (ids == r0).astype(F32)
    is1 = (ids == r1).astype(F32)
    before = (
        lax.broadcasted_iota(jnp.int32, (toks, toks), 0)
        < lax.broadcasted_iota(jnp.int32, (toks, toks), 1)
    ).astype(F32).astype(BF)
    earlier = dot((is0 + is1).astype(BF), before, 1, 0)
    pos0 = r0.astype(F32) * cap + jnp.sum(is0 * earlier, axis=0, keepdims=True)
    pos1 = r1.astype(F32) * cap + jnp.sum(is1 * earlier, axis=0, keepdims=True)
    slot = lax.broadcasted_iota(jnp.int32, (groups * cap, toks), 0).astype(F32)
    m0 = (slot == pos0).astype(F32)
    m1 = (slot == pos1).astype(F32)
    pick[...] = (m0 + m1).astype(BF)
    both[:, 0:toks] = m0.astype(BF)
    both[:, toks:] = m1.astype(BF)

    sub = lax.broadcasted_iota(jnp.int32, (8, toks), 0)
    spos[...] = jnp.where(sub == 0, pos0, jnp.where(sub == 1, pos1, -1.0))
    outer = lax.rem(me, 2) == me // (groups // 2)
    heads = range(2, groups, 2)

    def rows_of(k, start, count):
        return pl.ds(pl.multiple_of(partner[k] * cap + start, 16), count)

    def to_expert(src, dst, kind, rsem, k):
        part = pl.ds(0, base if src.shape[1] >= base else src.shape[1])
        return pltpu.make_async_remote_copy(
            src_ref=src.at[k, part], dst_ref=dst.at[k, part],
            send_sem=z_ss.at[kind], recv_sem=rsem.at[k - 1],
            device_id={"expert": partner[k]}, device_id_type=MESH)

    def all_sent(ref, sem):
        pltpu.make_async_remote_copy(
            src_ref=ref, dst_ref=ref, send_sem=sem, recv_sem=sem,
            device_id={"dp": peer[1]}, device_id_type=MESH).wait_send()

    def all_got(ref, sem):
        pltpu.make_async_remote_copy(
            src_ref=ref, dst_ref=ref, send_sem=sem, recv_sem=sem,
            device_id={"dp": peer[1]}, device_id_type=MESH).wait_recv()

    d_copy, o_copy = {}, {}
    step = 512

    def far_copy(k, c):
        return pltpu.make_async_remote_copy(
            src_ref=tok_ref.at[:, pl.ds(c * step, step)], dst_ref=far.at[k // 2 - 1, :, pl.ds(c * step, step)],
            send_sem=f_ss.at[0], recv_sem=f_rs.at[k // 2 - 1, c],
            device_id={"expert": partner[k]}, device_id_type=MESH)

    def pos_copy(k):
        return pltpu.make_async_remote_copy(
            src_ref=spos, dst_ref=fpos.at[k // 2 - 1], send_sem=f_ss.at[1], recv_sem=p_rs.at[k // 2 - 1],
            device_id={"expert": partner[k]}, device_id_type=MESH)

    def relay_copy(k, c):
        cols = pl.ds(c * step, step)
        return pltpu.make_async_remote_copy(
            src_ref=rel.at[k // 2 - 1, :, cols], dst_ref=rx.at[k + 1, :, cols],
            send_sem=f_ss.at[2], recv_sem=q_rs.at[k // 2 - 1],
            device_id={"expert": partner[1]}, device_id_type=MESH)

    def send_far():
        for k in heads:
            for c in range(features // step):
                far_copy(k, c).start()
    sequence = list(range(groups))
    load_t.wait()
    greeted = False
    for k in [1, 2] + [1] + sequence[3:] + [0]:
        count = base if k else cap
        if k == 0 or not greeted:
            dest = sx if k else rx
            for c in range(0, features, step):
                dest[k, 0:count, c : c + step] = dot(
                    pick[rows_of(k, 0, count), :], tok_ref[:, c : c + step], 1, 0).astype(BF)
        if not greeted:
            with jax.named_scope("p_barrier"):
                pl.semaphore_wait(barrier, groups - 1 + ways - 1)
            for far_k in heads:
                pos_copy(far_k).start()
            send_far()
        if not greeted:
            greeted = True
            x_copy = to_expert(sx, rx, 0, x_rs, k)
            pl.when(jnp.logical_not(outer))(x_copy.start)
            load_d.wait()
            sides[0:toks, :] = gh_ref[:, 0, :]
            sides[toks:, :] = gh_ref[:, 1, :]
            continue
        if k == 1:
            pl.when(outer)(x_copy.start)
        dest = sd if k else rd
        dest[k, 0:count, :] = dot(both[rows_of(k, 0, count), :], sides[...], 1, 0).astype(BF)
        if k:
            d_copy[k] = to_expert(sd, rd, 1, d_rs, k)
            d_copy[k].start()
            over = rows_of(k, base, cap - base)
            so[k, :, wide_x:] = fold(extra, dot(both[over, :], sides[...], 1, 0))
            if k == 1:
                so[k, :, 0:wide_x] = fold(extra, dot(pick[over, :], tok_ref[...], 1, 0))
                o_copy[k] = to_expert(so, ro, 2, o_rs, k)
            else:
                cols = pl.ds(wide_x, so.shape[2] - wide_x)
                o_copy[k] = pltpu.make_async_remote_copy(
                    src_ref=so.at[k, :, cols], dst_ref=ro.at[k, :, cols],
                    send_sem=z_ss.at[5], recv_sem=o_rs.at[k - 1],
                    device_id={"expert": partner[k]}, device_id_type=MESH)
            o_copy[k].start()

    tile = 256

    def place(mask):
        return pl.ds(mask * cap, cap)

    def part_cols(part):
        return pl.ds(part * hidden, hidden)

    def delta_copy(k, mask, part):
        bit = via[mask, part]
        return pltpu.make_async_remote_copy(
            src_ref=dg.at[k, place(mask ^ (1 << bit)), part_cols(part)],
            dst_ref=dg.at[k, place(mask), part_cols(part)],
            send_sem=c_ss.at[0],
            recv_sem=c_rs.at[k, passed.index((mask, part)) if (mask, part) in passed else len(passed)],
            device_id={"dp": peer[1 << bit]}, device_id_type=MESH)

    def rows_copy(k, mask):
        start = pl.multiple_of(peer[mask] * block, block)
        return pltpu.make_async_remote_copy(
            src_ref=rx.at[k, :, pl.ds(start, block)],
            dst_ref=xg.at[k, place(mask)],
            send_sem=g_ss.at[0], recv_sem=g_rs.at[k],
            device_id={"dp": peer[mask]}, device_id_type=MESH)

    b_copy = {k: to_expert(sback, ret, 3, b_rs, k) for k in sequence[1:]}
    e_copy = {k: to_expert(sbo, rbo, 4, e_rs, k) for k in sequence[1:]}

    def give_back(k):
        b_copy[k].start()
        e_copy[k].start()

    waited = set()

    def arrive(k, mask, part):
        if mask and (k, mask, part) not in waited:
            waited.add((k, mask, part))
            delta_copy(k, mask, part).wait_recv()

    def pass_on(k, level):
        steps = [(m, part) for part in range(2) for m in masks if bin(m).count("1") == level]
        steps.sort(key=lambda step: (via[step] == 0, step[1] != step[0] // (ways // 2)))
        for mask, part in steps:
            arrive(k, mask ^ (1 << via[mask, part]), part)
            delta_copy(k, mask, part).start()

    def relay(k):
        h = k // 2 - 1
        with jax.named_scope(f"p_pos{k}"):
            pos_copy(k).wait_recv()
        slots = lax.broadcasted_iota(jnp.int32, (cap, toks), 0)
        for which, owner in enumerate((me, partner[1])):
            here = (slots + owner * cap).astype(F32)
            pfar[which] = (
                (here == fpos[h, 0:1, :]).astype(F32) + (here == fpos[h, 1:2, :]).astype(F32)
            ).astype(BF)
        for c in range(features // step):
            with jax.named_scope(f"p_far{k}_{c}"):
                far_copy(k, c).wait_recv()
            cols = pl.ds(c * step, step)
            rel[h, :, cols] = dot(pfar[1], far[h, :, cols], 1, 0).astype(BF)
            relay_copy(k, c).start()
            rx[k, :, cols] = dot(pfar[0], far[h, :, cols], 1, 0).astype(BF)
        for mask in masks[::-1]:
            rows_copy(k, mask).start()

    def compute(k):
        if k:
            with jax.named_scope(f"p_x{k}"):
                if k == 1:
                    x_copy.wait_recv()
                elif k % 2:
                    all_got(rx.at[k], q_rs.at[k // 2 - 1])
            with jax.named_scope(f"p_d{k}"):
                d_copy[k].wait_recv()
                o_copy[k].wait_recv()
            if k == 1:
                rx[k, base:cap, :] = unfold(extra, ro[k, :, 0:wide_x], features)
            rd[k, base:cap, :] = unfold(extra, ro[k, :, wide_x:], hidden)
        if k < 2 or k % 2:
            for mask in masks[::-1]:
                rows_copy(k, mask).start()
        if k == 0:
            load_g.wait()
            load_u.wait()

        def forward(f, carry):
            cols = pl.ds(pl.multiple_of(f * tile, tile), tile)
            ucols = pl.ds(pl.multiple_of(f * tile + hidden, tile), tile)
            x = rx[k]
            gate = dot(x, wg[:, cols], 1, 0)
            up = dot(x, wu[:, cols], 1, 0)
            sig = jax.nn.sigmoid(gate)
            grad = rd[k, :, cols].astype(F32)
            dg[k, 0:cap, cols] = (grad * up * sig * (1.0 + gate * (1.0 - sig))).astype(BF)
            dg[k, 0:cap, ucols] = (grad * gate * sig).astype(BF)
            return carry

        with jax.named_scope(f"p_fwd{k}"):
            lax.fori_loop(0, hidden // tile, forward, 0)
        pass_on(k, 1)
        held = sback if k else ret

        def backward(d, carry):
            cols = pl.ds(pl.multiple_of(d * tile, tile), tile)
            held[k, :, cols] = (
                dot(dg[k, 0:cap, 0:hidden], wg[cols, :], 1, 1)
                + dot(dg[k, 0:cap, hidden:], wu[cols, :], 1, 1)
            ).astype(BF)
            return carry

        with jax.named_scope(f"p_back{k}"):
            lax.fori_loop(0, features // tile, backward, 0)
        if k:
            sbo[k] = fold(extra, sback[k, base:cap, :].astype(F32))
            if k > 1:
                give_back(k)
        start = pl.multiple_of(dp * block, block)
        xg[k, 0:cap, :] = rx[k, :, pl.ds(start, block)]

    def weight(k):
        with jax.named_scope(f"p_got{k}"):
            all_got(xg.at[k, pl.ds(cap, (ways - 1) * cap)], g_rs.at[k])
            for mask, part in passed:
                arrive(k, mask, part)
            leaves = 2 * (ways - 1) - len(passed)
            all_got(dg.at[k, pl.ds(0, leaves * cap), part_cols(0)], c_rs.at[k, len(passed)])
        for part in range(2):
            value = dot(xg[k], dg[k, :, part * hidden : (part + 1) * hidden], 0, 0)
            if k == sequence[0]:
                acc[part] = value
            elif k != sequence[-1]:
                acc[part] += value
            else:
                (out_gate, out_up)[part][...] = acc[part] + value

    def hop(at, level):
        if 0 <= at < groups:
            with jax.named_scope(f"p_pass{sequence[at]}_{level}"):
                pass_on(sequence[at], level)

    compute(0)
    before = set(waited)

    @pl.when(jnp.logical_not(outer))
    def _():
        relay(2)
        hop(0, 2)
        compute(2)
        hop(0, 3)
        compute(1)
        give_back(1)
        hop(2, 2)

    after = set(waited)
    waited.clear()
    waited.update(before)

    @pl.when(outer)
    def _():
        compute(1)
        hop(0, 2)
        relay(2)
        hop(1, 2)
        hop(0, 3)
        compute(2)
        give_back(1)

    both_ways = after & waited
    after = after | waited
    waited.clear()
    waited.update(both_ways)
    compute(3)
    before = set(waited)

    @pl.when(jnp.logical_not(outer))
    def _():
        hop(1, 2)

    waited.clear()
    waited.update(before)

    @pl.when(outer)
    def _():
        hop(2, 2)

    waited.update(after)

    def tokens_back(k):
        if k:
            with jax.named_scope(f"p_ret{k}"):
                b_copy[k].wait_recv()
                e_copy[k].wait_recv()
            ret[k, base:cap, :] = unfold(extra, rbo[k], features)
        for c in range(0, features, step):
            total = dot(pick[rows_of(k, 0, cap), :], ret[k, :, c : c + step], 0, 0)
            if k:
                total = tot[:, c : c + step] + total
            if k == sequence[-1]:
                out_tok[:, c : c + step] = total.astype(BF)
            else:
                tot[:, c : c + step] = total

    hop(1, 3)
    weight(0)
    hop(2, 3)
    tokens_back(0)
    hop(3, 2)
    weight(1)
    hop(3, 3)
    weight(2)
    tokens_back(1)
    tokens_back(2)
    weight(3)
    tokens_back(3)

    with jax.named_scope("p_drain"):
        all_sent(sx.at[1], z_ss.at[0])
        all_sent(so.at[1], z_ss.at[2])
        for kind, ref in ((1, sd), (3, sback), (4, sbo)):
            all_sent(ref.at[pl.ds(1, groups - 1), pl.ds(0, min(base, ref.shape[1]))], z_ss.at[kind])
        all_sent(so.at[pl.ds(2, groups - 2), pl.ds(0, 16), pl.ds(wide_x, so.shape[2] - wide_x)], z_ss.at[5])
        for _ in heads:
            all_sent(tok_ref, f_ss.at[0])
            all_sent(spos, f_ss.at[1])
        all_sent(rel, f_ss.at[2])
        all_sent(xg.at[pl.ds(0, groups), pl.ds(cap, (ways - 1) * cap)], g_ss.at[0])
        all_sent(dg.at[pl.ds(0, groups), pl.ds(cap, (ways - 1) * cap)], c_ss.at[0])


def flush_kernel(tok, gate, up, out_tok, out_gate, out_up, sems):
    copies = [
        pltpu.make_async_copy(src, dst, sems.at[i])
        for i, (src, dst) in enumerate(((tok, out_tok), (gate, out_gate), (up, out_up)))
    ]
    for copy in copies:
        copy.start()
    for copy in copies:
        copy.wait()


def pin(array):
    return pltpu.with_memory_space_constraint(array, pltpu.HBM)


def per_device(tokens, routes, grad_hidden, w_gate, w_up):
    tok_rows, features = tokens.shape
    per_token = routes.shape[1]
    hidden = w_gate.shape[2]
    groups = lax.axis_size("expert")
    ways = lax.axis_size("dp")
    pair_count = tok_rows * per_token
    cold_most = pair_count // groups
    cold_floor = cold_most - 2 - cold_most // 8
    hot_total = pair_count - (groups - 3) * cold_floor - cold_most
    hot_most = (hot_total + 1) // 2 + min((hot_total - 2 * cold_most - 2) // 2, cold_most // 4)
    cap = (max(hot_most, cold_most) + 15) // 16 * 16
    slots = groups * cap
    block = features // ways
    bits = ways.bit_length() - 1
    hops = len(rs_plan(bits)[1])
    half = ways // 2
    vmem = pl.BlockSpec(memory_space=pltpu.VMEM)
    hbm = pl.BlockSpec(memory_space=pl.ANY)
    dma = pltpu.SemaphoreType.DMA
    base = max(hot_most, cold_most) // 16 * 16
    extra = max(hot_most, cold_most) - base
    held = 2 * (
        2 * features * hidden + 3 * slots * tok_rows + 5 * slots * (features + hidden)
        + ways * slots * (2 * hidden + block) + groups * tok_rows * (features + 4 * hidden)
    ) + 4 * 4 * block * hidden
    if groups == 4 and bits == 3 and 8 <= extra and features <= 2048 and held < 9 << 22:
        far = pl.BlockSpec(memory_space=pltpu.HBM)
        over = fold_width(extra, features)
        shapes = (
            jax.ShapeDtypeStruct((tok_rows, features), BF),
            jax.ShapeDtypeStruct((block, hidden), F32),
            jax.ShapeDtypeStruct((block, hidden), F32),
        )
        results = pl.pallas_call(
            functools.partial(gather_kernel, groups, ways, cap, base, extra),
            out_shape=shapes,
            in_specs=[far] * 5,
            out_specs=(vmem, vmem, vmem),
            scratch_shapes=[
                pltpu.VMEM((per_token, tok_rows), jnp.int32),
                pltpu.VMEM((tok_rows, features), BF),
                pltpu.VMEM((tok_rows, per_token, hidden), BF),
                pltpu.VMEM((features, hidden), BF),
                pltpu.VMEM((features, hidden), BF),
                pltpu.VMEM((slots, tok_rows), BF),
                pltpu.VMEM((slots, 2 * tok_rows), BF),
                pltpu.VMEM((2 * tok_rows, hidden), BF),
                pltpu.VMEM((2, base, features), BF),
                pltpu.VMEM((groups, base, hidden), BF),
                pltpu.VMEM((groups, 16, over + fold_width(extra, hidden)), BF),
                pltpu.VMEM((groups, cap, features), BF),
                pltpu.VMEM((groups, cap, hidden), BF),
                pltpu.VMEM((groups, 16, over + fold_width(extra, hidden)), BF),
                pltpu.VMEM((8, tok_rows), F32),
                pltpu.VMEM((groups // 2 - 1, 8, tok_rows), F32),
                pltpu.VMEM((groups // 2 - 1, tok_rows, features), BF),
                pltpu.VMEM((2, cap, tok_rows), BF),
                pltpu.VMEM((groups // 2 - 1, cap, features), BF),
                pltpu.VMEM((groups, ways * cap, 2 * hidden), BF),
                pltpu.VMEM((groups, ways * cap, block), BF),
                pltpu.VMEM((groups, cap, features), BF),
                pltpu.VMEM((groups, 16, over), BF),
                pltpu.VMEM((groups, cap, features), BF),
                pltpu.VMEM((groups, 16, over), BF),
                pltpu.VMEM((tok_rows, features), F32),
                pltpu.VMEM((2, block, hidden), F32),
                dma((5,)),
                dma((3,)),
                dma((groups // 2 - 1, features // 512)),
                dma((groups // 2 - 1,)),
                dma((groups // 2 - 1,)),
                dma((6,)),
                dma((1,)),
            ] + [dma((groups - 1,))] * 4 + [dma((1,)), dma((groups,)), dma((1,)), dma((groups, ways - 1))],
            compiler_params=pltpu.CompilerParams(
                collective_id=0, has_side_effects=True, vmem_limit_bytes=10 << 22),
        )(pin(routes.T), pin(tokens), pin(grad_hidden), pin(w_gate[0]), pin(w_up[0]))
        tok_grad, gate_grad, up_grad = pl.pallas_call(
            flush_kernel,
            out_shape=shapes,
            in_specs=[vmem] * 3,
            out_specs=(far,) * 3,
            scratch_shapes=[dma((3,))],
            compiler_params=pltpu.CompilerParams(vmem_limit_bytes=1 << 20),
        )(*results)
        return tok_grad, gate_grad[None], up_grad[None]
    tok_grad, gate_grad, up_grad = pl.pallas_call(
        functools.partial(kernel, groups, ways, cap),
        out_shape=(
            jax.ShapeDtypeStruct((tok_rows, features), BF),
            jax.ShapeDtypeStruct((block, hidden), F32),
            jax.ShapeDtypeStruct((block, hidden), F32),
        ),
        in_specs=[vmem, vmem, vmem, vmem, hbm, hbm],
        out_specs=(vmem, vmem, vmem),
        scratch_shapes=[
            pltpu.VMEM((features, hidden), BF),
            pltpu.VMEM((features, hidden), BF),
            pltpu.VMEM((slots, tok_rows), BF),
            pltpu.VMEM((slots, features + hidden), BF),
            pltpu.VMEM((slots, features + hidden), BF),
            pltpu.VMEM((slots, 2 * hidden), BF),
            pltpu.VMEM((slots, features), BF),
            pltpu.VMEM((slots, features), BF),
            pltpu.VMEM((half, block, 2 * hidden), BF),
            pltpu.VMEM((half, block, 2 * hidden), BF),
            pltpu.VMEM((hops, block, hidden), BF),
            pltpu.VMEM((hops, block, hidden), BF),
            pltpu.VMEM((2, half, block, hidden), F32),
            dma((2,)),
            dma((groups,)),
            dma((groups,)),
            dma((groups,)),
            dma((groups,)),
            dma((half,)),
            dma((half,)),
            dma((hops,)),
            dma((hops,)),
        ],
        compiler_params=pltpu.CompilerParams(collective_id=0, has_side_effects=True),
    )(tokens, routes.T, grad_hidden[:, 0], grad_hidden[:, 1], w_gate[0], w_up[0])
    return tok_grad, gate_grad[None], up_grad[None]


def solution(mesh):
    placed = (
        P(("dp", "expert"), None),
        P(("dp", "expert"), None),
        P(("dp", "expert"), None, None),
        P("expert", None, None),
        P("expert", None, None),
    )
    return jax.shard_map(
        per_device,
        mesh=mesh,
        in_specs=placed,
        out_specs=(P(("dp", "expert"), None), P("expert", "dp", None), P("expert", "dp", None)),
        check_vma=False,
    )
```

```python
import functools

import jax
import jax.numpy as jnp
from jax import lax
from jax.experimental import pallas as pl
from jax.experimental.pallas import tpu as pltpu
from jax.sharding import PartitionSpec as P

MESH = pl.DeviceIdType.MESH
BF = jnp.bfloat16
F32 = jnp.float32


def dot(a, b, da, db):
    return lax.dot_general(a, b, (((da,), (db,)), ((), ())), preferred_element_type=F32)


def rs_plan(bits):
    orders = (tuple(range(bits)), (0,) + tuple(range(bits - 1, 0, -1)))
    index = {}
    for which, order in enumerate(orders):
        done = 1
        for bit in order[1:]:
            flag = 1 << bit
            for mask in range(1 << bits):
                if mask & done or mask & flag:
                    continue
                index[which, bit, mask] = len(index)
            done |= flag
    return orders, index


def kernel(
    groups, ways, cap, tok_ref, rt_ref, gh0_ref, gh1_ref, wg_hbm, wu_hbm,
    out_tok, out_gate, out_up,
    wg, wu, pick, send, rows, delta, back, ret, core_send, core_recv, hop_send, hop_recv, acc,
    w_sem, z_ssem, z_rsem, b_ssem, b_rsem, c_ssem, c_rsem, h_ssem, h_rsem,
):
    features = tok_ref.shape[1]
    toks = tok_ref.shape[0]
    hidden = gh0_ref.shape[1]
    block = features // ways
    bits = ways.bit_length() - 1
    orders, index = rs_plan(bits)
    me = lax.axis_index("expert")
    dp = lax.axis_index("dp")
    my_bits = [lax.rem(dp // (1 << b), 2) for b in range(bits)]

    def peer_dp(mask):
        total = 0
        for b in range(bits):
            bit = 1 - my_bits[b] if mask >> b & 1 else my_bits[b]
            total = total + bit * (1 << b)
        return total

    load_g = pltpu.make_async_copy(wg_hbm, wg, w_sem.at[0])
    load_u = pltpu.make_async_copy(wu_hbm, wu, w_sem.at[1])
    load_g.start()
    load_u.start()

    barrier = pltpu.get_barrier_semaphore()
    for off in range(1, groups):
        pl.semaphore_signal(
            barrier, inc=1, device_id={"expert": lax.rem(me + off, groups)}, device_id_type=MESH
        )
    for b in range(bits):
        pl.semaphore_signal(
            barrier, inc=1, device_id={"dp": peer_dp(1 << b)}, device_id_type=MESH
        )

    r0 = rt_ref[0:1, :]
    r1 = rt_ref[1:2, :]
    wide = max(groups, 8)
    ids = lax.broadcasted_iota(jnp.int32, (wide, toks), 0)
    is0 = (ids == r0).astype(F32)
    is1 = (ids == r1).astype(F32)
    before = (
        lax.broadcasted_iota(jnp.int32, (toks, toks), 0)
        < lax.broadcasted_iota(jnp.int32, (toks, toks), 1)
    ).astype(F32).astype(BF)
    earlier = dot((is0 + is1).astype(BF), before, 1, 0)
    pos0 = r0.astype(F32) * cap + jnp.sum(is0 * earlier, axis=0, keepdims=True)
    pos1 = r1.astype(F32) * cap + jnp.sum(is1 * earlier, axis=0, keepdims=True)
    slot = lax.broadcasted_iota(jnp.int32, (groups * cap, toks), 0).astype(F32)
    m0 = (slot == pos0).astype(F32)
    m1 = (slot == pos1).astype(F32)
    pick[...] = (m0 + m1).astype(BF)
    send[:, features:] = (
        dot(m0.astype(BF), gh0_ref[...], 1, 0) + dot(m1.astype(BF), gh1_ref[...], 1, 0)
    ).astype(BF)
    step = 512
    for c in range(0, features, step):
        send[:, c : c + step] = dot(pick[...], tok_ref[:, c : c + step], 1, 0).astype(BF)

    pl.semaphore_wait(barrier, groups - 1 + bits)

    def span(i):
        return pl.ds(pl.multiple_of(i * cap, cap), cap)

    def exchange(src, dst, ssem, rsem):
        sends, recvs = [], []
        for off in range(1, groups):
            to = lax.rem(me + off, groups)
            frm = lax.rem(me + groups - off, groups)
            sends.append(pltpu.make_async_remote_copy(
                src_ref=src.at[span(to)], dst_ref=dst.at[span(me)],
                send_sem=ssem.at[off], recv_sem=rsem.at[off],
                device_id={"expert": to}, device_id_type=MESH))
            recvs.append(pltpu.make_async_remote_copy(
                src_ref=src.at[span(frm)], dst_ref=dst.at[span(frm)],
                send_sem=ssem.at[off], recv_sem=rsem.at[off],
                device_id={"expert": frm}, device_id_type=MESH))
        for copy in sends:
            copy.start()
        return sends, recvs

    out_sends, out_recvs = exchange(send, rows, z_ssem, z_rsem)
    rows[span(me), :] = send[span(me), :]
    load_g.wait()
    load_u.wait()
    for copy in out_recvs:
        copy.wait_recv()

    tile = 256

    def forward(f, carry):
        cols = pl.ds(pl.multiple_of(f * tile, tile), tile)
        ucols = pl.ds(pl.multiple_of(f * tile + hidden, tile), tile)
        dcols = pl.ds(pl.multiple_of(f * tile + features, tile), tile)
        x = rows[:, 0:features]
        gate = dot(x, wg[:, cols], 1, 0)
        up = dot(x, wu[:, cols], 1, 0)
        sig = jax.nn.sigmoid(gate)
        grad = rows[:, dcols].astype(F32)
        delta[:, cols] = (grad * up * sig * (1.0 + gate * (1.0 - sig))).astype(BF)
        delta[:, ucols] = (grad * gate * sig).astype(BF)
        return carry

    lax.fori_loop(0, hidden // tile, forward, 0)

    def weight_block(mask):
        start = pl.multiple_of(peer_dp(mask) * block, block)
        return dot(rows[:, pl.ds(start, block)], delta[...], 0, 0)

    core_sends = {}
    for mask in range(ways - 1, 0, -2):
        place = mask >> 1
        core_send[place] = weight_block(mask).astype(BF)
        copy = pltpu.make_async_remote_copy(
            src_ref=core_send.at[place], dst_ref=core_recv.at[place],
            send_sem=c_ssem.at[place], recv_sem=c_rsem.at[place],
            device_id={"dp": peer_dp(1)}, device_id_type=MESH)
        copy.start()
        core_sends[place] = copy

    def backward(d, carry):
        cols = pl.ds(pl.multiple_of(d * tile, tile), tile)
        back[:, cols] = (
            dot(delta[:, 0:hidden], wg[cols, :], 1, 1)
            + dot(delta[:, hidden:], wu[cols, :], 1, 1)
        ).astype(BF)
        return carry

    lax.fori_loop(0, features // tile, backward, 0)
    back_sends, back_recvs = exchange(back, ret, b_ssem, b_rsem)
    ret[span(me), :] = back[span(me), :]

    hop_sends = []

    def hop(which, bit, mask, value):
        at = index[which, bit, mask ^ (1 << bit)]
        hop_send[at] = value.astype(BF)
        copy = pltpu.make_async_remote_copy(
            src_ref=hop_send.at[at], dst_ref=hop_recv.at[at],
            send_sem=h_ssem.at[at], recv_sem=h_rsem.at[at],
            device_id={"dp": peer_dp(1 << bit)}, device_id_type=MESH)
        copy.start()
        hop_sends.append(copy)

    def arrived(which, bit, mask):
        at = index[which, bit, mask]
        pltpu.make_async_remote_copy(
            src_ref=hop_send.at[at], dst_ref=hop_recv.at[at],
            send_sem=h_ssem.at[at], recv_sem=h_rsem.at[at],
            device_id={"dp": peer_dp(1 << bit)}, device_id_type=MESH).wait_recv()
        return hop_recv[at].astype(F32)

    for mask in range(ways - 2, -1, -2):
        place = mask >> 1
        core_sends[place].wait_recv()
        total = weight_block(mask) + core_recv[place].astype(F32)
        for which in range(2):
            part = total[:, which * hidden : (which + 1) * hidden]
            bit = orders[which][1]
            if mask >> bit & 1:
                hop(which, bit, mask, part)
            else:
                acc[which, place] = part

    for level in range(2, bits):
        for mask in range(ways - 2, -1, -2):
            for which in range(2):
                order = orders[which]
                fixed = sum(1 << b for b in order[:level])
                if mask & fixed:
                    continue
                value = acc[which, mask >> 1] + arrived(which, order[level - 1], mask)
                if mask >> order[level] & 1:
                    hop(which, order[level], mask, value)
                else:
                    acc[which, mask >> 1] = value

    for copy in back_recvs:
        copy.wait_recv()
    for c in range(0, features, step):
        out_tok[:, c : c + step] = dot(pick[...], ret[:, c : c + step], 0, 0).astype(BF)
    out_gate[...] = acc[0, 0] + arrived(0, orders[0][-1], 0)
    out_up[...] = acc[1, 0] + arrived(1, orders[1][-1], 0)

    for copy in out_sends + back_sends + list(core_sends.values()) + hop_sends:
        copy.wait_send()


def gather_plan(bits):
    if bits > 2:
        orders = (tuple(range(1, bits)) + (0,), tuple(range(bits - 1, 0, -1)) + (0,))
    else:
        orders = (tuple(range(bits - 1, -1, -1)),) * 2
    via = {}
    for part, order in enumerate(orders):
        for mask in range(1, 1 << bits):
            via[mask, part] = [b for b in order if mask >> b & 1][-1]
    masks = sorted(range(1, 1 << bits), key=lambda mask: (bin(mask).count("1"), mask))
    return masks, via


def fold_width(extra, width):
    return width // 2 + (extra - 8) * 128


def fold(extra, rows):
    width = rows.shape[1]
    parts = [jnp.concatenate([rows[0:8, : width // 2], rows[0:8, width // 2 :]], axis=0)]
    sub = lax.broadcasted_iota(jnp.int32, (16, 128), 0)
    for j in range(8, extra):
        total = jnp.zeros((16, 128), F32)
        for c in range(width // 128):
            total = jnp.where(sub == c, rows[j : j + 1, c * 128 : (c + 1) * 128], total)
        parts.append(total)
    return jnp.concatenate([p.astype(BF) for p in parts], axis=1)


def unfold(extra, folded, width):
    rows = folded.astype(F32)
    top = jnp.concatenate([rows[0:8, : width // 2], rows[8:16, : width // 2]], axis=1)
    sub = lax.broadcasted_iota(jnp.int32, (8, width), 0)
    low = jnp.zeros((8, width), F32)
    for j in range(8, extra):
        at = width // 2 + (j - 8) * 128
        row = jnp.concatenate(
            [rows[c : c + 1, at : at + 128] for c in range(width // 128)], axis=1)
        low = jnp.where(sub == j - 8, row, low)
    return jnp.concatenate([top, low], axis=0).astype(BF)


def gather_kernel(
    groups, ways, cap, base, extra, rt_hbm, tok_hbm, gh_hbm, wg_hbm, wu_hbm,
    out_tok, out_gate, out_up,
    rt_ref, tok_ref, gh_ref, wg, wu, pick, both, sides, sx, sd, so, rx, rd, ro, spos, fpos, far, pfar, rel, dg, xg, sback, sbo, ret, rbo, tot, acc,
    l_sem, f_ss, f_rs, p_rs, q_rs, z_ss, x_rs, d_rs, o_rs, b_rs, e_rs, g_ss, g_rs, c_ss, c_rs,
):
    toks, features = tok_ref.shape
    hidden = gh_ref.shape[2]
    wide_x = fold_width(extra, features)
    block = features // ways
    bits = ways.bit_length() - 1
    masks, via = gather_plan(bits)
    passed = sorted({(m ^ (1 << bit), part) for (m, part), bit in via.items()} - {(0, 0), (0, 1)})
    me = lax.axis_index("expert")
    dp = lax.axis_index("dp")

    def flip(value, mask, count):
        total = 0
        for b in range(count):
            bit = lax.rem(value // (1 << b), 2)
            if mask >> b & 1:
                bit = 1 - bit
            total = total + bit * (1 << b)
        return total

    partner = [flip(me, k, groups.bit_length() - 1) for k in range(groups)]
    peer = [flip(dp, m, bits) for m in range(ways)]

    load_r = pltpu.make_async_copy(rt_hbm, rt_ref, l_sem.at[4])
    load_r.start()
    load_t = pltpu.make_async_copy(tok_hbm, tok_ref, l_sem.at[0])
    load_d = pltpu.make_async_copy(gh_hbm, gh_ref, l_sem.at[1])
    load_g = pltpu.make_async_copy(wg_hbm, wg, l_sem.at[2])
    load_u = pltpu.make_async_copy(wu_hbm, wu, l_sem.at[3])
    load_t.start()
    load_d.start()
    load_g.start()
    load_u.start()

    barrier = pltpu.get_barrier_semaphore()
    for k in range(1, groups):
        pl.semaphore_signal(barrier, inc=1, device_id={"expert": partner[k]}, device_id_type=MESH)
    for m in range(1, ways):
        pl.semaphore_signal(barrier, inc=1, device_id={"dp": peer[m]}, device_id_type=MESH)

    load_r.wait()
    r0 = rt_ref[0:1, :]
    r1 = rt_ref[1:2, :]
    wide = max(groups, 8)
    ids = lax.broadcasted_iota(jnp.int32, (wide, toks), 0)
    is0 = (ids == r0).astype(F32)
    is1 = (ids == r1).astype(F32)
    before = (
        lax.broadcasted_iota(jnp.int32, (toks, toks), 0)
        < lax.broadcasted_iota(jnp.int32, (toks, toks), 1)
    ).astype(F32).astype(BF)
    earlier = dot((is0 + is1).astype(BF), before, 1, 0)
    pos0 = r0.astype(F32) * cap + jnp.sum(is0 * earlier, axis=0, keepdims=True)
    pos1 = r1.astype(F32) * cap + jnp.sum(is1 * earlier, axis=0, keepdims=True)
    slot = lax.broadcasted_iota(jnp.int32, (groups * cap, toks), 0).astype(F32)
    m0 = (slot == pos0).astype(F32)
    m1 = (slot == pos1).astype(F32)
    pick[...] = (m0 + m1).astype(BF)
    both[:, 0:toks] = m0.astype(BF)
    both[:, toks:] = m1.astype(BF)

    sub = lax.broadcasted_iota(jnp.int32, (8, toks), 0)
    spos[...] = jnp.where(sub == 0, pos0, jnp.where(sub == 1, pos1, -1.0))
    outer = lax.rem(me, 2) == me // (groups // 2)
    heads = range(2, groups, 2)

    def rows_of(k, start, count):
        return pl.ds(pl.multiple_of(partner[k] * cap + start, 16), count)

    def to_expert(src, dst, kind, rsem, k):
        part = pl.ds(0, base if src.shape[1] >= base else src.shape[1])
        return pltpu.make_async_remote_copy(
            src_ref=src.at[k, part], dst_ref=dst.at[k, part],
            send_sem=z_ss.at[kind], recv_sem=rsem.at[k - 1],
            device_id={"expert": partner[k]}, device_id_type=MESH)

    def all_sent(ref, sem):
        pltpu.make_async_remote_copy(
            src_ref=ref, dst_ref=ref, send_sem=sem, recv_sem=sem,
            device_id={"dp": peer[1]}, device_id_type=MESH).wait_send()

    def all_got(ref, sem):
        pltpu.make_async_remote_copy(
            src_ref=ref, dst_ref=ref, send_sem=sem, recv_sem=sem,
            device_id={"dp": peer[1]}, device_id_type=MESH).wait_recv()

    d_copy, o_copy = {}, {}
    step = 512

    def far_copy(k, c):
        return pltpu.make_async_remote_copy(
            src_ref=tok_ref.at[:, pl.ds(c * step, step)], dst_ref=far.at[k // 2 - 1, :, pl.ds(c * step, step)],
            send_sem=f_ss.at[0], recv_sem=f_rs.at[k // 2 - 1, c],
            device_id={"expert": partner[k]}, device_id_type=MESH)

    def pos_copy(k):
        return pltpu.make_async_remote_copy(
            src_ref=spos, dst_ref=fpos.at[k // 2 - 1], send_sem=f_ss.at[1], recv_sem=p_rs.at[k // 2 - 1],
            device_id={"expert": partner[k]}, device_id_type=MESH)

    def relay_copy(k, c):
        cols = pl.ds(c * step, step)
        return pltpu.make_async_remote_copy(
            src_ref=rel.at[k // 2 - 1, :, cols], dst_ref=rx.at[k + 1, :, cols],
            send_sem=f_ss.at[2], recv_sem=q_rs.at[k // 2 - 1],
            device_id={"expert": partner[1]}, device_id_type=MESH)

    def send_far():
        for k in heads:
            for c in range(features // step):
                far_copy(k, c).start()
    sequence = list(range(groups))
    load_t.wait()
    greeted = False
    for k in [1, 2] + [1] + sequence[3:] + [0]:
        count = base if k else cap
        if k == 0 or not greeted:
            dest = sx if k else rx
            for c in range(0, features, step):
                dest[k, 0:count, c : c + step] = dot(
                    pick[rows_of(k, 0, count), :], tok_ref[:, c : c + step], 1, 0).astype(BF)
        if not greeted:
            with jax.named_scope("p_barrier"):
                pl.semaphore_wait(barrier, groups - 1 + ways - 1)
            for far_k in heads:
                pos_copy(far_k).start()
            send_far()
        if not greeted:
            greeted = True
            x_copy = to_expert(sx, rx, 0, x_rs, k)
            pl.when(jnp.logical_not(outer))(x_copy.start)
            load_d.wait()
            sides[0:toks, :] = gh_ref[:, 0, :]
            sides[toks:, :] = gh_ref[:, 1, :]
            continue
        if k == 1:
            pl.when(outer)(x_copy.start)
        dest = sd if k else rd
        dest[k, 0:count, :] = dot(both[rows_of(k, 0, count), :], sides[...], 1, 0).astype(BF)
        if k:
            d_copy[k] = to_expert(sd, rd, 1, d_rs, k)
            d_copy[k].start()
            over = rows_of(k, base, cap - base)
            so[k, :, wide_x:] = fold(extra, dot(both[over, :], sides[...], 1, 0))
            if k == 1:
                so[k, :, 0:wide_x] = fold(extra, dot(pick[over, :], tok_ref[...], 1, 0))
                o_copy[k] = to_expert(so, ro, 2, o_rs, k)
            else:
                cols = pl.ds(wide_x, so.shape[2] - wide_x)
                o_copy[k] = pltpu.make_async_remote_copy(
                    src_ref=so.at[k, :, cols], dst_ref=ro.at[k, :, cols],
                    send_sem=z_ss.at[5], recv_sem=o_rs.at[k - 1],
                    device_id={"expert": partner[k]}, device_id_type=MESH)
            o_copy[k].start()

    tile = 256

    def place(mask):
        return pl.ds(mask * cap, cap)

    def part_cols(part):
        return pl.ds(part * hidden, hidden)

    def delta_copy(k, mask, part):
        bit = via[mask, part]
        return pltpu.make_async_remote_copy(
            src_ref=dg.at[k, place(mask ^ (1 << bit)), part_cols(part)],
            dst_ref=dg.at[k, place(mask), part_cols(part)],
            send_sem=c_ss.at[0],
            recv_sem=c_rs.at[k, passed.index((mask, part)) if (mask, part) in passed else len(passed)],
            device_id={"dp": peer[1 << bit]}, device_id_type=MESH)

    def rows_copy(k, mask):
        start = pl.multiple_of(peer[mask] * block, block)
        return pltpu.make_async_remote_copy(
            src_ref=rx.at[k, :, pl.ds(start, block)],
            dst_ref=xg.at[k, place(mask)],
            send_sem=g_ss.at[0], recv_sem=g_rs.at[k],
            device_id={"dp": peer[mask]}, device_id_type=MESH)

    b_copy = {k: to_expert(sback, ret, 3, b_rs, k) for k in sequence[1:]}
    e_copy = {k: to_expert(sbo, rbo, 4, e_rs, k) for k in sequence[1:]}

    def give_back(k):
        b_copy[k].start()
        e_copy[k].start()

    waited = set()

    def arrive(k, mask, part):
        if mask and (k, mask, part) not in waited:
            waited.add((k, mask, part))
            delta_copy(k, mask, part).wait_recv()

    def pass_on(k, level):
        steps = [(m, part) for part in range(2) for m in masks if bin(m).count("1") == level]
        steps.sort(key=lambda step: (via[step] == 0, step[1] != step[0] // (ways // 2)))
        for mask, part in steps:
            arrive(k, mask ^ (1 << via[mask, part]), part)
            delta_copy(k, mask, part).start()

    def relay(k):
        h = k // 2 - 1
        with jax.named_scope(f"p_pos{k}"):
            pos_copy(k).wait_recv()
        slots = lax.broadcasted_iota(jnp.int32, (cap, toks), 0)
        for which, owner in enumerate((me, partner[1])):
            here = (slots + owner * cap).astype(F32)
            pfar[which] = (
                (here == fpos[h, 0:1, :]).astype(F32) + (here == fpos[h, 1:2, :]).astype(F32)
            ).astype(BF)
        for c in range(features // step):
            with jax.named_scope(f"p_far{k}_{c}"):
                far_copy(k, c).wait_recv()
            cols = pl.ds(c * step, step)
            rel[h, :, cols] = dot(pfar[1], far[h, :, cols], 1, 0).astype(BF)
            relay_copy(k, c).start()
            rx[k, :, cols] = dot(pfar[0], far[h, :, cols], 1, 0).astype(BF)
        for mask in masks[::-1]:
            rows_copy(k, mask).start()

    def compute(k):
        if k:
            with jax.named_scope(f"p_x{k}"):
                if k == 1:
                    x_copy.wait_recv()
                elif k % 2:
                    all_got(rx.at[k], q_rs.at[k // 2 - 1])
            with jax.named_scope(f"p_d{k}"):
                d_copy[k].wait_recv()
                o_copy[k].wait_recv()
            if k == 1:
                rx[k, base:cap, :] = unfold(extra, ro[k, :, 0:wide_x], features)
            rd[k, base:cap, :] = unfold(extra, ro[k, :, wide_x:], hidden)
        if k < 2 or k % 2:
            for mask in masks[::-1]:
                rows_copy(k, mask).start()
        if k == 0:
            load_g.wait()
            load_u.wait()

        def forward(f, carry):
            cols = pl.ds(pl.multiple_of(f * tile, tile), tile)
            ucols = pl.ds(pl.multiple_of(f * tile + hidden, tile), tile)
            x = rx[k]
            gate = dot(x, wg[:, cols], 1, 0)
            up = dot(x, wu[:, cols], 1, 0)
            sig = jax.nn.sigmoid(gate)
            grad = rd[k, :, cols].astype(F32)
            dg[k, 0:cap, cols] = (grad * up * sig * (1.0 + gate * (1.0 - sig))).astype(BF)
            dg[k, 0:cap, ucols] = (grad * gate * sig).astype(BF)
            return carry

        with jax.named_scope(f"p_fwd{k}"):
            lax.fori_loop(0, hidden // tile, forward, 0)
        pass_on(k, 1)
        held = sback if k else ret

        def backward(d, carry):
            cols = pl.ds(pl.multiple_of(d * tile, tile), tile)
            held[k, :, cols] = (
                dot(dg[k, 0:cap, 0:hidden], wg[cols, :], 1, 1)
                + dot(dg[k, 0:cap, hidden:], wu[cols, :], 1, 1)
            ).astype(BF)
            return carry

        with jax.named_scope(f"p_back{k}"):
            lax.fori_loop(0, features // tile, backward, 0)
        if k:
            sbo[k] = fold(extra, sback[k, base:cap, :].astype(F32))
            if k > 1:
                give_back(k)
        start = pl.multiple_of(dp * block, block)
        xg[k, 0:cap, :] = rx[k, :, pl.ds(start, block)]

    def weight(k):
        with jax.named_scope(f"p_got{k}"):
            all_got(xg.at[k, pl.ds(cap, (ways - 1) * cap)], g_rs.at[k])
            for mask, part in passed:
                arrive(k, mask, part)
            leaves = 2 * (ways - 1) - len(passed)
            all_got(dg.at[k, pl.ds(0, leaves * cap), part_cols(0)], c_rs.at[k, len(passed)])
        for part in range(2):
            value = dot(xg[k], dg[k, :, part * hidden : (part + 1) * hidden], 0, 0)
            if k == sequence[0]:
                acc[part] = value
            elif k != sequence[-1]:
                acc[part] += value
            else:
                (out_gate, out_up)[part][...] = acc[part] + value

    def hop(at, level):
        if 0 <= at < groups:
            with jax.named_scope(f"p_pass{sequence[at]}_{level}"):
                pass_on(sequence[at], level)

    compute(0)
    before = set(waited)

    @pl.when(jnp.logical_not(outer))
    def _():
        relay(2)
        hop(0, 2)
        compute(2)
        hop(0, 3)
        compute(1)
        give_back(1)
        hop(2, 2)

    after = set(waited)
    waited.clear()
    waited.update(before)

    @pl.when(outer)
    def _():
        compute(1)
        hop(0, 2)
        relay(2)
        hop(1, 2)
        hop(0, 3)
        compute(2)
        give_back(1)

    both_ways = after & waited
    after = after | waited
    waited.clear()
    waited.update(both_ways)
    compute(3)
    before = set(waited)

    @pl.when(jnp.logical_not(outer))
    def _():
        hop(1, 2)

    waited.clear()
    waited.update(before)

    @pl.when(outer)
    def _():
        hop(2, 2)

    waited.update(after)

    def tokens_back(k):
        if k:
            with jax.named_scope(f"p_ret{k}"):
                b_copy[k].wait_recv()
                e_copy[k].wait_recv()
            ret[k, base:cap, :] = unfold(extra, rbo[k], features)
        for c in range(0, features, step):
            total = dot(pick[rows_of(k, 0, cap), :], ret[k, :, c : c + step], 0, 0)
            if k:
                total = tot[:, c : c + step] + total
            if k == sequence[-1]:
                out_tok[:, c : c + step] = total.astype(BF)
            else:
                tot[:, c : c + step] = total

    hop(3, 2)
    hop(1, 3)
    hop(2, 3)
    weight(0)
    tokens_back(0)
    weight(1)
    hop(3, 3)
    weight(2)
    tokens_back(1)
    tokens_back(2)
    weight(3)
    tokens_back(3)

    with jax.named_scope("p_drain"):
        all_sent(sx.at[1], z_ss.at[0])
        all_sent(so.at[1], z_ss.at[2])
        for kind, ref in ((1, sd), (3, sback), (4, sbo)):
            all_sent(ref.at[pl.ds(1, groups - 1), pl.ds(0, min(base, ref.shape[1]))], z_ss.at[kind])
        all_sent(so.at[pl.ds(2, groups - 2), pl.ds(0, 16), pl.ds(wide_x, so.shape[2] - wide_x)], z_ss.at[5])
        for _ in heads:
            all_sent(tok_ref, f_ss.at[0])
            all_sent(spos, f_ss.at[1])
        all_sent(rel, f_ss.at[2])
        all_sent(xg.at[pl.ds(0, groups), pl.ds(cap, (ways - 1) * cap)], g_ss.at[0])
        all_sent(dg.at[pl.ds(0, groups), pl.ds(cap, (ways - 1) * cap)], c_ss.at[0])


def flush_kernel(tok, gate, up, out_tok, out_gate, out_up, sems):
    copies = [
        pltpu.make_async_copy(src, dst, sems.at[i])
        for i, (src, dst) in enumerate(((tok, out_tok), (gate, out_gate), (up, out_up)))
    ]
    for copy in copies:
        copy.start()
    for copy in copies:
        copy.wait()


def pin(array):
    return pltpu.with_memory_space_constraint(array, pltpu.HBM)


def per_device(tokens, routes, grad_hidden, w_gate, w_up):
    tok_rows, features = tokens.shape
    per_token = routes.shape[1]
    hidden = w_gate.shape[2]
    groups = lax.axis_size("expert")
    ways = lax.axis_size("dp")
    pair_count = tok_rows * per_token
    cold_most = pair_count // groups
    cold_floor = cold_most - 2 - cold_most // 8
    hot_total = pair_count - (groups - 3) * cold_floor - cold_most
    hot_most = (hot_total + 1) // 2 + min((hot_total - 2 * cold_most - 2) // 2, cold_most // 4)
    cap = (max(hot_most, cold_most) + 15) // 16 * 16
    slots = groups * cap
    block = features // ways
    bits = ways.bit_length() - 1
    hops = len(rs_plan(bits)[1])
    half = ways // 2
    vmem = pl.BlockSpec(memory_space=pltpu.VMEM)
    hbm = pl.BlockSpec(memory_space=pl.ANY)
    dma = pltpu.SemaphoreType.DMA
    base = max(hot_most, cold_most) // 16 * 16
    extra = max(hot_most, cold_most) - base
    held = 2 * (
        2 * features * hidden + 3 * slots * tok_rows + 5 * slots * (features + hidden)
        + ways * slots * (2 * hidden + block) + groups * tok_rows * (features + 4 * hidden)
    ) + 4 * 4 * block * hidden
    if groups == 4 and bits == 3 and 8 <= extra and features <= 2048 and held < 9 << 22:
        far = pl.BlockSpec(memory_space=pltpu.HBM)
        over = fold_width(extra, features)
        shapes = (
            jax.ShapeDtypeStruct((tok_rows, features), BF),
            jax.ShapeDtypeStruct((block, hidden), F32),
            jax.ShapeDtypeStruct((block, hidden), F32),
        )
        results = pl.pallas_call(
            functools.partial(gather_kernel, groups, ways, cap, base, extra),
            out_shape=shapes,
            in_specs=[far] * 5,
            out_specs=(vmem, vmem, vmem),
            scratch_shapes=[
                pltpu.VMEM((per_token, tok_rows), jnp.int32),
                pltpu.VMEM((tok_rows, features), BF),
                pltpu.VMEM((tok_rows, per_token, hidden), BF),
                pltpu.VMEM((features, hidden), BF),
                pltpu.VMEM((features, hidden), BF),
                pltpu.VMEM((slots, tok_rows), BF),
                pltpu.VMEM((slots, 2 * tok_rows), BF),
                pltpu.VMEM((2 * tok_rows, hidden), BF),
                pltpu.VMEM((2, base, features), BF),
                pltpu.VMEM((groups, base, hidden), BF),
                pltpu.VMEM((groups, 16, over + fold_width(extra, hidden)), BF),
                pltpu.VMEM((groups, cap, features), BF),
                pltpu.VMEM((groups, cap, hidden), BF),
                pltpu.VMEM((groups, 16, over + fold_width(extra, hidden)), BF),
                pltpu.VMEM((8, tok_rows), F32),
                pltpu.VMEM((groups // 2 - 1, 8, tok_rows), F32),
                pltpu.VMEM((groups // 2 - 1, tok_rows, features), BF),
                pltpu.VMEM((2, cap, tok_rows), BF),
                pltpu.VMEM((groups // 2 - 1, cap, features), BF),
                pltpu.VMEM((groups, ways * cap, 2 * hidden), BF),
                pltpu.VMEM((groups, ways * cap, block), BF),
                pltpu.VMEM((groups, cap, features), BF),
                pltpu.VMEM((groups, 16, over), BF),
                pltpu.VMEM((groups, cap, features), BF),
                pltpu.VMEM((groups, 16, over), BF),
                pltpu.VMEM((tok_rows, features), F32),
                pltpu.VMEM((2, block, hidden), F32),
                dma((5,)),
                dma((3,)),
                dma((groups // 2 - 1, features // 512)),
                dma((groups // 2 - 1,)),
                dma((groups // 2 - 1,)),
                dma((6,)),
                dma((1,)),
            ] + [dma((groups - 1,))] * 4 + [dma((1,)), dma((groups,)), dma((1,)), dma((groups, ways - 1))],
            compiler_params=pltpu.CompilerParams(
                collective_id=0, has_side_effects=True, vmem_limit_bytes=10 << 22),
        )(pin(routes.T), pin(tokens), pin(grad_hidden), pin(w_gate[0]), pin(w_up[0]))
        tok_grad, gate_grad, up_grad = pl.pallas_call(
            flush_kernel,
            out_shape=shapes,
            in_specs=[vmem] * 3,
            out_specs=(far,) * 3,
            scratch_shapes=[dma((3,))],
            compiler_params=pltpu.CompilerParams(vmem_limit_bytes=1 << 20),
        )(*results)
        return tok_grad, gate_grad[None], up_grad[None]
    tok_grad, gate_grad, up_grad = pl.pallas_call(
        functools.partial(kernel, groups, ways, cap),
        out_shape=(
            jax.ShapeDtypeStruct((tok_rows, features), BF),
            jax.ShapeDtypeStruct((block, hidden), F32),
            jax.ShapeDtypeStruct((block, hidden), F32),
        ),
        in_specs=[vmem, vmem, vmem, vmem, hbm, hbm],
        out_specs=(vmem, vmem, vmem),
        scratch_shapes=[
            pltpu.VMEM((features, hidden), BF),
            pltpu.VMEM((features, hidden), BF),
            pltpu.VMEM((slots, tok_rows), BF),
            pltpu.VMEM((slots, features + hidden), BF),
            pltpu.VMEM((slots, features + hidden), BF),
            pltpu.VMEM((slots, 2 * hidden), BF),
            pltpu.VMEM((slots, features), BF),
            pltpu.VMEM((slots, features), BF),
            pltpu.VMEM((half, block, 2 * hidden), BF),
            pltpu.VMEM((half, block, 2 * hidden), BF),
            pltpu.VMEM((hops, block, hidden), BF),
            pltpu.VMEM((hops, block, hidden), BF),
            pltpu.VMEM((2, half, block, hidden), F32),
            dma((2,)),
            dma((groups,)),
            dma((groups,)),
            dma((groups,)),
            dma((groups,)),
            dma((half,)),
            dma((half,)),
            dma((hops,)),
            dma((hops,)),
        ],
        compiler_params=pltpu.CompilerParams(collective_id=0, has_side_effects=True),
    )(tokens, routes.T, grad_hidden[:, 0], grad_hidden[:, 1], w_gate[0], w_up[0])
    return tok_grad, gate_grad[None], up_grad[None]


def solution(mesh):
    placed = (
        P(("dp", "expert"), None),
        P(("dp", "expert"), None),
        P(("dp", "expert"), None, None),
        P("expert", None, None),
        P("expert", None, None),
    )
    return jax.shard_map(
        per_device,
        mesh=mesh,
        in_specs=placed,
        out_specs=(P(("dp", "expert"), None), P("expert", "dp", None), P("expert", "dp", None)),
        check_vma=False,
    )
```
